256 devices in a mesh: tm: 64 (over z, y, core), mp: 4 (over x).
Axes of the slice: x: 4, y: 4, z: 8, core: 2. Of those that a mesh axis runs over, the one named last changes fastest.
Arguments:
- latents: float32 [4, 64, 4, 4096], P(None, 'tm'), may hold values from -6 to 6
- noise: float32 [4, 64, 4, 4096], P(None, 'tm'), may hold values from -6 to 6
- start_step: int32 [4], replicated, may hold values from 64 to 999
- slide: int32 [4], replicated, may hold values from 1 to 64, as said below
- w_in: float32 [4, 320], replicated, may hold values from -3 to 3
- w_gate: bfloat16 [320, 1280], P(None, 'mp'), may hold values from -0.3125 to 0.3125
- w_value: bfloat16 [320, 1280], P(None, 'mp'), may hold values from -0.3125 to 0.3125
- w_down: bfloat16 [1280, 320], P('mp'), may hold values from -0.15625 to 0.15625
- w_out: float32 [320, 4], replicated, may hold values from -0.3125 to 0.3125
Outputs:
- next_window: float32 [4, 64, 4, 4096], P(None, 'tm')
- eps: float32 [4, 64, 4, 4096], P(None, 'tm', None, 'mp')
The draws below stay inside these ranges and needn't reach their ends.
Inputs may be any that keep to these rules, and one draw needn't show every extreme that they name: `slide`: some prompt slides by exactly 64, and another by exactly 1.
All inputs are finite; a program needn't handle non-finite values.
Results may differ from the reference program's by a relative error of at most 0.0023.
Values sent between devices are 32-bit elements; how exact they have to be, the bound alone decides.
A program may use at most 64 MiB of HBM per device.

```python
import math
import jax
import jax.numpy as jnp
from jax import lax

C = 320
FF = 1280
LAT = 4
POS = 4096
PROMPTS = 4
TSTEPS = 1000
WIN = 64
SMAX = 64


def draw_slide(key, part):
    first, second = jax.random.split(jax.random.fold_in(key, 17))
    values = jax.random.randint(first, (PROMPTS,), 1, SMAX + 1)
    order = jax.random.permutation(second, PROMPTS)
    values = jnp.where(order == 0, SMAX, values)
    values = jnp.where(order == 1, 1, values)
    return values.astype(jnp.int32)


def plant(array, own_key, low, top_value):
    longest = array.shape.index(max(array.shape))
    spots = []
    for shift in (0, 1):
        where = [jax.random.randint(jax.random.fold_in(own_key, axis), (), 0, length) for axis, length in enumerate(array.shape)]
        where[longest] = (where[longest] + shift) % array.shape[longest]
        spots.append(tuple(where))
    return array.at[spots[0]].set(low).at[spots[1]].set(top_value)


def block_levels(key, dims, cuts, least, largest):
    level, own = 1.0, jax.random.fold_in(key, 6)
    for position, shards_of in cuts:
        steps = jnp.exp(jax.random.uniform(jax.random.fold_in(own, position), (shards_of,), jnp.float32, least / len(cuts), largest / len(cuts)))
        level = level * jnp.repeat(steps, dims[position] // shards_of).reshape([-1 if axis == position else 1 for axis in range(len(dims))])
    return level


def bell_draw(rng, extent, deviation, bound, pieces=(), kind=jnp.bfloat16):
    loudness = block_levels(rng, extent, pieces, -0.22, 0.18) if pieces else 1.0
    entries = jax.random.normal(rng, extent, jnp.float32) * deviation * loudness
    return jnp.minimum(jnp.maximum(entries, -bound), bound).astype(kind)


def setup_inputs(seed: int = 0) -> dict:
    splits = jax.random.split(jax.random.key(seed), 10)
    latents = bell_draw(splits[0], (PROMPTS, WIN, LAT, POS), 1.0, 6.0, ((1, 64),), jnp.float32)
    noise = bell_draw(splits[1], (PROMPTS, WIN, LAT, POS), 1.0, 6.0, ((1, 64),), jnp.float32)
    start_step = plant(jax.random.randint(splits[2], (PROMPTS,), WIN, TSTEPS), jax.random.fold_in(splits[2], 1), WIN, TSTEPS - 1).astype(jnp.int32)
    slide = draw_slide(jax.random.fold_in(splits[9], 71), 0)
    w_in = bell_draw(splits[4], (LAT, C), LAT ** -0.5, 3.0, (), jnp.float32)
    w_gate = bell_draw(splits[5], (C, FF), C ** -0.5, 0.3125, ((1, 4),))
    w_value = bell_draw(splits[6], (C, FF), C ** -0.5, 0.3125, ((1, 4),))
    w_down = bell_draw(splits[7], (FF, C), FF ** -0.5, 0.15625, ((0, 4),))
    w_out = bell_draw(splits[8], (C, LAT), C ** -0.5, 0.3125, (), jnp.float32)
    return {"latents": latents, "noise": noise, "start_step": start_step, "slide": slide, "w_in": w_in, "w_gate": w_gate, "w_value": w_value, "w_down": w_down, "w_out": w_out}


def plan():
    steps_f = jnp.arange(TSTEPS, dtype=jnp.float32)
    beta = 0.0001 + (0.02 - 0.0001) * steps_f / (TSTEPS - 1)
    abar = jnp.cumprod(1.0 - beta)
    return (beta, abar)

def embed(times):
    half = C // 2
    freq = jnp.exp(-math.log(10000.0) * jnp.arange(half, dtype=jnp.float32) / half)
    angle = times[..., None] * freq
    return jnp.concatenate([jnp.cos(angle), jnp.sin(angle)], axis=-1)

def reference(latents, noise, start_step, slide, w_in, w_gate, w_value, w_down, w_out):
    beta, abar = plan()
    slots = jnp.arange(WIN, dtype=jnp.int32)
    times = start_step[:, None] - slots[None, :]
    beta_t = beta[times][:, :, None, None]
    abar_t = abar[times][:, :, None, None]
    emb = embed(times.astype(jnp.float32)).reshape(PROMPTS * WIN, C)
    items = latents.reshape(PROMPTS * WIN, LAT, POS)

    def denoise(pair):
        latent, vector = pair
        hid = jnp.dot(w_in.T, latent, precision=lax.Precision.HIGHEST) + vector[:, None]
        mean = lax.optimization_barrier(jnp.mean(hid, axis=0))
        var = lax.optimization_barrier(jnp.mean((hid - mean) ** 2, axis=0))
        normed = ((hid - mean) * lax.rsqrt(var + 1e-05)).astype(jnp.bfloat16)
        gate = jnp.dot(w_gate.T, normed, preferred_element_type=jnp.float32)
        value = jnp.dot(w_value.T, normed, preferred_element_type=jnp.float32)
        hidden = (jax.nn.gelu(gate, approximate=False) * value).astype(jnp.bfloat16)
        branch = jnp.dot(w_down.T, hidden, preferred_element_type=jnp.float32)
        return jnp.dot(w_out.T, hid + branch, precision=lax.Precision.HIGHEST)
    eps = lax.map(denoise, (items, emb)).reshape(PROMPTS, WIN, LAT, POS)
    stepped = (latents - beta_t / jnp.sqrt(1.0 - abar_t) * eps) / jnp.sqrt(1.0 - beta_t) + jnp.sqrt(beta_t) * noise
    drift = stepped - latents
    updated = latents[:, :1] + (jnp.cumsum(drift, axis=1) - drift)
    source = jnp.minimum(slots[None, :] + slide[:, None], WIN - 1).astype(jnp.int32)
    next_window = jnp.take_along_axis(updated, source[:, :, None, None], axis=1)
    return (next_window, eps)
```

```python
import functools
import math

import jax
import jax.numpy as jnp
from jax import lax
from jax.experimental import pallas as pl
from jax.experimental.pallas import tpu as pltpu
from jax.sharding import PartitionSpec as P

TSTEPS = 1000
TILE = 512
SLOTS = 64
HIGHEST = lax.Precision.HIGHEST
MESH = pl.DeviceIdType.MESH


def split3(x):
    high = x.astype(jnp.bfloat16).astype(jnp.float32)
    rest = x - high
    mid = rest.astype(jnp.bfloat16).astype(jnp.float32)
    return high, mid, rest - mid


def contract_last(a, b):
    return lax.dot_general(
        a, b, (((1,), (1,)), ((), ())), precision=HIGHEST, preferred_element_type=jnp.float32
    )


def product_all(x):
    for axis, extent in ((1, 128), (0, 8)):
        step = 1
        while step < extent:
            x = x * pltpu.roll(x, step, axis)
            step *= 2
    return x


def scanner_of(prompt, lat):
    return (2 * lat + prompt % 2) * 8 + 2 * prompt + 1


def sweep(
    start, slide, lat_ref, noise_ref, w_in_ref, w_gate_ref, w_value_ref, w_down_ref, w_out_ref,
    out_ref, eps_ref,
    lhs, down, base_row, gram, coef, part, part_in, drift, slots_in, sums, picked, whole,
    part_send, part_recv, one_send, one_recv, two_send, two_recv, all_send, all_recv,
):
    prompts, _, lats, pos = lat_ref.shape
    channels = w_in_ref.shape[1]
    hidden = w_gate_ref.shape[1]
    share = pos // 4
    i = lax.axis_index("tm")
    m = lax.axis_index("mp")

    barrier = pltpu.get_barrier_semaphore()

    def greet(k, carry):
        pl.semaphore_signal(
            barrier, inc=1, device_id={"tm": lax.rem(i + k, SLOTS), "mp": m}, device_id_type=MESH
        )
        return carry

    for k in (1, 2, 3):
        pl.semaphore_signal(
            barrier, inc=1, device_id={"tm": i, "mp": lax.rem(m + k, 4)}, device_id_type=MESH
        )
    lax.fori_loop(1, SLOTS, greet, 0)

    row8 = lax.broadcasted_iota(jnp.int32, (8, channels), 0)
    lane8 = lax.broadcasted_iota(jnp.int32, (8, channels), 1)
    half = channels // 2
    steps = jnp.zeros((8, channels), jnp.int32)
    for p in range(prompts):
        steps = jnp.where(row8 == 4 + p, start[p] - i, steps)
    freq = jnp.exp(
        -math.log(10000.0) * jnp.where(lane8 < half, lane8, lane8 - half).astype(jnp.float32) / half
    )
    angle = steps.astype(jnp.float32) * freq
    emb = jnp.where(lane8 < half, jnp.cos(angle), jnp.sin(angle))
    w_in = w_in_ref[...]
    rows = jnp.where(row8 < 4, jnp.concatenate([w_in, w_in], axis=0), emb)
    centred = rows - jnp.mean(rows, axis=1, keepdims=True)
    gram[...] = contract_last(centred, centred) * (1.0 / channels)

    w_out = jnp.concatenate(
        [w_out_ref[...], jnp.zeros((channels, 124), jnp.float32)], axis=1
    )
    w_out_t = jnp.transpose(w_out)[:8, :]
    base_row[...] = contract_last(w_out_t, rows)

    def three_rows(x):
        return jnp.concatenate(split3(x) + (jnp.zeros_like(x),), axis=0).astype(jnp.bfloat16)

    lefts = three_rows(centred)
    tables = []
    for w_ref in (w_gate_ref, w_value_ref):
        pieces = jnp.dot(lefts, w_ref[...], preferred_element_type=jnp.float32)
        tables.append((pieces[0:8] + pieces[8:16] + pieces[16:24]) * math.sqrt(0.5))
    pieces = lax.dot_general(
        three_rows(w_out_t), w_down_ref[...], (((1,), (1,)), ((), ())),
        preferred_element_type=jnp.float32,
    )
    folded = pieces[0:8] + pieces[8:16] + pieces[16:24]
    high, mid, low = split3(folded)
    down[...] = jnp.concatenate([high, mid, low, jnp.zeros_like(low)], axis=0).astype(jnp.bfloat16)

    rowk = lax.broadcasted_iota(jnp.int32, (8, hidden), 0)
    for p in range(prompts):
        for q, table in enumerate(tables):
            own = jnp.where(
                rowk < 4, table, jnp.where(rowk == 4, table[4 + p : 5 + p, :], 0.0)
            )
            high, mid, low = split3(own)
            stack = jnp.concatenate(
                [high, high, mid, mid, high, low, jnp.zeros((80, hidden), jnp.float32)], axis=0
            )
            lhs[p, q * hidden : (q + 1) * hidden, :] = jnp.transpose(stack).astype(jnp.bfloat16)

    grid = (
        lax.broadcasted_iota(jnp.int32, (8, 128), 0) * 128
        + lax.broadcasted_iota(jnp.int32, (8, 128), 1)
    )

    def beta_at(k):
        return 0.0001 + (0.02 - 0.0001) * k.astype(jnp.float32) / (TSTEPS - 1)

    kept = 1.0 - beta_at(grid)
    for p in range(prompts):
        t = jnp.full((8, 128), start[p] - i, jnp.int32)
        abar = product_all(jnp.where(grid <= t, kept, 1.0))
        beta = beta_at(t)
        coef[p, 0] = beta / jnp.sqrt(1.0 - abar)
        coef[p, 1] = 1.0 / jnp.sqrt(1.0 - beta)
        coef[p, 2] = jnp.sqrt(beta)

    rowt = lax.broadcasted_iota(jnp.int32, (8, TILE), 0)

    def denoise(p):
        cov = gram[...]
        left = lhs[p]
        inner = down[...]

        def tile(n, carry):
            off = pl.multiple_of(n * TILE, TILE)
            x4 = lat_ref[p, 0, :, pl.ds(off, TILE)]
            x8 = jnp.concatenate([x4, x4], axis=0)
            x = jnp.where(rowt < 4, x8, 0.0)
            z = jnp.zeros((8, TILE), jnp.float32) + 2.0 * cov[:, 4 + p : 5 + p]
            for b in range(4):
                z = z + cov[:, b : b + 1] * x4[b : b + 1, :]
            var = jnp.sum(x * z, axis=0, keepdims=True) + cov[4 + p : 5 + p, 4 + p : 5 + p]
            scale = lax.rsqrt(var + 1e-05)
            y = jnp.where(rowt < 4, x8, jnp.where(rowt == 4, 1.0, 0.0)) * scale
            high, mid, low = split3(y)
            right = jnp.concatenate(
                [high, mid, high, mid, low, high, jnp.zeros((80, TILE), jnp.float32)], axis=0
            ).astype(jnp.bfloat16)
            both = jnp.dot(left, right, preferred_element_type=jnp.float32)
            g = both[:hidden]
            v = both[hidden:]
            act = (g * v * (1.0 + lax.erf(g))).astype(jnp.bfloat16)
            got = jnp.dot(inner, act, preferred_element_type=jnp.float32)
            got = got[0:8] + got[8:16] + got[16:24]
            per = share // TILE
            part[p, n // per, :, pl.ds(pl.multiple_of(lax.rem(n, per) * TILE, TILE), TILE)] = got[0:4]
            return carry

        lax.fori_loop(0, pos // TILE, tile, 0)

    def send_parts(p):
        for k in (1, 2, 3):
            peer = lax.rem(m + k, 4)
            pltpu.make_async_remote_copy(
                src_ref=part.at[p, peer], dst_ref=part_in.at[p, k - 1],
                send_sem=part_send, recv_sem=part_recv.at[p],
                device_id={"tm": i, "mp": peer}, device_id_type=MESH,
            ).start()

    def finish(p):
        pltpu.make_async_copy(part_in.at[p], part_in.at[p], part_recv.at[p]).wait()
        total = part[p, m] + part_in[p, 0] + part_in[p, 1] + part_in[p, 2]
        mine = pl.ds(pl.multiple_of(m * share, share), share)
        cur = lat_ref[p, 0, :, mine]
        nz = noise_ref[p, 0, :, mine]
        for a in range(4):
            total = total + base_row[0:4, a : a + 1] * cur[a : a + 1, :]
        total = total + base_row[0:4, 4 + p : 5 + p]
        eps_ref[p, 0] = total
        c1 = coef[p, 0][0:4]
        c2 = coef[p, 1][0:4]
        c3 = coef[p, 2][0:4]
        head = jnp.where(jnp.full((4, 128), i, jnp.int32) == 0, 1.0, 0.0)
        for s in range(8):
            lanes = slice(s * 128, (s + 1) * 128)
            term = (cur[:, lanes] - c1 * total[:, lanes]) * c2 + c3 * nz[:, lanes] - cur[:, lanes]
            drift[p, :, s, :] = term + head * cur[:, lanes]
        for a in range(lats):
            target = scanner_of(p, a)

            @pl.when(i != target)
            def _():
                pltpu.make_async_remote_copy(
                    src_ref=drift.at[p, a], dst_ref=slots_in.at[i],
                    send_sem=one_send, recv_sem=one_recv,
                    device_id={"tm": target, "mp": m}, device_id_type=MESH,
                ).start()

            @pl.when(i == target)
            def _():
                slots_in[SLOTS] = drift[p, a]

    pl_core = lax.rem(i, 2)
    my_prompt = lax.rem(i // 2, 4)
    my_z = i // 8
    my_lat = my_z // 2
    scanning = jnp.logical_and(pl_core == 1, lax.rem(my_z, 2) == lax.rem(my_prompt, 2))

    denoise(0)
    pl.semaphore_wait(barrier, SLOTS - 1 + 3)
    send_parts(0)
    for p in range(1, prompts):
        denoise(p)
        send_parts(p)
        finish(p - 1)
    finish(prompts - 1)

    @pl.when(scanning)
    def _():
        pltpu.make_async_copy(
            slots_in.at[pl.ds(0, SLOTS - 1)], slots_in.at[pl.ds(0, SLOTS - 1)], one_recv
        ).wait()
        slots_in[i] = slots_in[SLOTS]
        acc = slots_in[0]
        sums[1] = acc
        for j in range(1, SLOTS - 1):
            acc = acc + slots_in[j]
            sums[j + 1] = acc
        by = slide[my_prompt]
        for j in range(SLOTS):
            picked[j] = sums[jnp.minimum(j + by, SLOTS - 1)]

        def deliver(k, carry):
            peer = lax.rem(i + k, SLOTS)
            pltpu.make_async_remote_copy(
                src_ref=picked.at[peer], dst_ref=whole.at[my_prompt, m, my_lat],
                send_sem=two_send, recv_sem=two_recv.at[my_prompt],
                device_id={"tm": peer, "mp": m}, device_id_type=MESH,
            ).start()
            return carry

        lax.fori_loop(1, SLOTS, deliver, 0)
        whole[my_prompt, m, my_lat] = picked[i]

    for p in range(prompts):
        mine = jnp.logical_and(scanning, my_prompt == p)

        @pl.when(mine)
        def _():
            pltpu.make_async_copy(
                whole.at[p, m, pl.ds(0, lats - 1)], whole.at[p, m, pl.ds(0, lats - 1)], two_recv.at[p]
            ).wait()

        @pl.when(jnp.logical_not(mine))
        def _():
            pltpu.make_async_copy(whole.at[p, m], whole.at[p, m], two_recv.at[p]).wait()

        for k in (1, 2, 3):
            peer = lax.rem(m + k, 4)
            pltpu.make_async_remote_copy(
                src_ref=whole.at[p, m], dst_ref=whole.at[p, m],
                send_sem=all_send, recv_sem=all_recv.at[p],
                device_id={"tm": i, "mp": peer}, device_id_type=MESH,
            ).start()

    for p in range(prompts):
        pltpu.make_async_copy(
            whole.at[p, pl.ds(0, 3)], whole.at[p, pl.ds(0, 3)], all_recv.at[p]
        ).wait()
        for q in range(4):
            for s in range(8):
                out_ref[p, 0, :, q * share + s * 128 : q * share + (s + 1) * 128] = whole[p, q, :, s, :]

    def settle(ref, sem):
        pltpu.make_async_copy(ref, ref, sem).wait()

    settle(part_in, part_send)
    settle(whole.at[:, pl.ds(0, 3)], all_send)

    @pl.when(scanning)
    def _():
        settle(slots_in.at[pl.ds(0, SLOTS - 1)], two_send)
        settle(slots_in.at[pl.ds(0, prompts * lats - 1)], one_send)

    @pl.when(jnp.logical_not(scanning))
    def _():
        settle(slots_in.at[pl.ds(0, prompts * lats)], one_send)


def shards(latents, noise, start_step, slide, w_in, w_gate, w_value, w_down, w_out):
    prompts, _, lats, pos = latents.shape
    hidden = w_gate.shape[1]
    share = pos // 4
    f32 = jnp.float32
    smem = pl.BlockSpec(memory_space=pltpu.SMEM)
    vmem = pl.BlockSpec(memory_space=pltpu.VMEM)
    dma = pltpu.SemaphoreType.DMA
    return pl.pallas_call(
        sweep,
        out_shape=(
            jax.ShapeDtypeStruct(latents.shape, f32),
            jax.ShapeDtypeStruct((prompts, 1, lats, share), f32),
        ),
        in_specs=[smem, smem] + [vmem] * 7,
        out_specs=(vmem, vmem),
        scratch_shapes=[
            pltpu.VMEM((prompts, 2 * hidden, 128), jnp.bfloat16),
            pltpu.VMEM((32, hidden), jnp.bfloat16),
            pltpu.VMEM((8, 8), f32),
            pltpu.VMEM((8, 8), f32),
            pltpu.VMEM((prompts, 3, 8, 128), f32),
            pltpu.VMEM((prompts, 4, lats, share), f32),
            pltpu.VMEM((prompts, 3, lats, share), f32),
            pltpu.VMEM((prompts, lats, 8, 128), f32),
            pltpu.VMEM((SLOTS + 1, 8, 128), f32),
            pltpu.VMEM((SLOTS, 8, 128), f32),
            pltpu.VMEM((SLOTS, 8, 128), f32),
            pltpu.VMEM((prompts, 4, lats, 8, 128), f32),
            dma, dma((prompts,)), dma, dma, dma, dma((prompts,)), dma, dma((prompts,)),
        ],
        compiler_params=pltpu.CompilerParams(collective_id=0, has_side_effects=True),
        name="sweep",
    )(start_step, slide, latents, noise, w_in, w_gate, w_value, w_down, w_out)


def solution(mesh):
    in_specs = (
        P(None, "tm", None, None),
        P(None, "tm", None, None),
        P(),
        P(),
        P(),
        P(None, "mp"),
        P(None, "mp"),
        P("mp", None),
        P(),
    )
    out_specs = (P(None, "tm", None, None), P(None, "tm", None, "mp"))
    return jax.shard_map(shards, mesh=mesh, in_specs=in_specs, out_specs=out_specs, check_vma=False)
```

```python
import functools
import math

import jax
import jax.numpy as jnp
from jax import lax
from jax.experimental import pallas as pl
from jax.experimental.pallas import tpu as pltpu
from jax.sharding import PartitionSpec as P

TSTEPS = 1000
TILE = 512
UNROLL = 8
SLOTS = 64
SCANNERS = 16
HIGHEST = lax.Precision.HIGHEST
MESH = pl.DeviceIdType.MESH


def split3(x):
    high = x.astype(jnp.bfloat16).astype(jnp.float32)
    rest = x - high
    mid = rest.astype(jnp.bfloat16).astype(jnp.float32)
    return high, mid, rest - mid


def contract_last(a, b):
    return lax.dot_general(
        a, b, (((1,), (1,)), ((), ())), precision=HIGHEST, preferred_element_type=jnp.float32
    )


def product_all(x):
    for axis, extent in ((1, 128), (0, 8)):
        step = 1
        while step < extent:
            x = x * pltpu.roll(x, step, axis)
            step *= 2
    return x


def sweep(
    start, slide, lat_ref, noise_ref, w_in_ref, w_gate_ref, w_value_ref, w_down_ref, w_out_ref,
    out_ref, eps_ref,
    lhs, down, base_row, gram, coef, part, part_in, drift, slots_in, sums, picked, whole,
    part_send, part_recv, one_send, one_recv, two_send, two_recv, all_send, all_recv,
):
    prompts, _, lats, pos = lat_ref.shape
    channels = w_in_ref.shape[1]
    hidden = w_gate_ref.shape[1]
    share = pos // 4
    i = lax.axis_index("tm")
    m = lax.axis_index("mp")

    barrier = pltpu.get_barrier_semaphore()

    def greet(k, carry):
        pl.semaphore_signal(
            barrier, inc=1, device_id={"tm": lax.rem(i + k, SLOTS), "mp": m}, device_id_type=MESH
        )
        return carry

    for k in (1, 2, 3):
        pl.semaphore_signal(
            barrier, inc=1, device_id={"tm": i, "mp": lax.rem(m + k, 4)}, device_id_type=MESH
        )

    @pl.when(i < SCANNERS)
    def _():
        lax.fori_loop(1, SLOTS, greet, 0)

    row8 = lax.broadcasted_iota(jnp.int32, (8, channels), 0)
    lane8 = lax.broadcasted_iota(jnp.int32, (8, channels), 1)
    half = channels // 2
    steps = jnp.zeros((8, channels), jnp.int32)
    for p in range(prompts):
        steps = jnp.where(row8 == 4 + p, start[p] - i, steps)
    freq = jnp.exp(
        -math.log(10000.0) * jnp.where(lane8 < half, lane8, lane8 - half).astype(jnp.float32) / half
    )
    angle = steps.astype(jnp.float32) * freq
    emb = jnp.where(lane8 < half, jnp.cos(angle), jnp.sin(angle))
    w_in = w_in_ref[...]
    rows = jnp.where(row8 < 4, jnp.concatenate([w_in, w_in], axis=0), emb)
    centred = rows - jnp.mean(rows, axis=1, keepdims=True)
    gram[...] = contract_last(centred, centred) * (1.0 / channels)

    w_out = w_out_ref[...]
    w_out_t = jnp.where(row8 < 4, jnp.concatenate([w_out, w_out], axis=0), 0.0)
    base_row[...] = contract_last(w_out_t, rows)

    def three_rows(x):
        return jnp.concatenate(split3(x) + (jnp.zeros_like(x),), axis=0).astype(jnp.bfloat16)

    rowk = lax.broadcasted_iota(jnp.int32, (8, hidden), 0)
    lefts = three_rows(centred)
    tables = []
    for w_ref in (w_gate_ref, w_value_ref):
        pieces = jnp.dot(lefts, w_ref[...], preferred_element_type=jnp.float32)
        tables.append((pieces[0:8] + pieces[8:16] + pieces[16:24]) * math.sqrt(0.5))
    pieces = lax.dot_general(
        three_rows(w_out_t), w_down_ref[...], (((1,), (1,)), ((), ())),
        preferred_element_type=jnp.float32,
    )
    folded = pieces[0:8] + pieces[8:16] + pieces[16:24]
    high, mid, low = split3(folded)
    down[...] = jnp.concatenate(
        [jnp.where(rowk < 4, high, pltpu.roll(mid, 4, 0)), low], axis=0
    ).astype(jnp.bfloat16)

    for p in range(prompts):
        for q, table in enumerate(tables):
            own = jnp.where(
                rowk < 4, table, jnp.where(rowk == 4, table[4 + p : 5 + p, :], 0.0)
            )
            high, mid, low = split3(own)
            stack = jnp.concatenate(
                [high, high, mid, mid, high, low, jnp.zeros((80, hidden), jnp.float32)], axis=0
            )
            lhs[p, q * hidden : (q + 1) * hidden, :] = jnp.transpose(stack).astype(jnp.bfloat16)

    grid = (
        lax.broadcasted_iota(jnp.int32, (8, 128), 0) * 128
        + lax.broadcasted_iota(jnp.int32, (8, 128), 1)
    )

    def beta_at(k):
        return 0.0001 + (0.02 - 0.0001) * k.astype(jnp.float32) / (TSTEPS - 1)

    kept = 1.0 - beta_at(grid)
    for p in range(prompts):
        t = jnp.full((8, 128), start[p] - i, jnp.int32)
        abar = product_all(jnp.where(grid <= t, kept, 1.0))
        beta = beta_at(t)
        coef[p, 0] = beta / jnp.sqrt(1.0 - abar)
        coef[p, 1] = 1.0 / jnp.sqrt(1.0 - beta)
        coef[p, 2] = jnp.sqrt(beta)

    rowt = lax.broadcasted_iota(jnp.int32, (8, TILE), 0)

    def denoise(p):
        cov = gram[...]
        left = lhs[p]
        inner = down[...]

        def tile(n, carry):
            off = pl.multiple_of(n * TILE, TILE)
            x4 = lat_ref[p, 0, :, pl.ds(off, TILE)]
            x8 = jnp.concatenate([x4, x4], axis=0)
            x = jnp.where(rowt < 4, x8, 0.0)
            z = jnp.zeros((8, TILE), jnp.float32) + 2.0 * cov[:, 4 + p : 5 + p]
            for b in range(4):
                z = z + cov[:, b : b + 1] * x4[b : b + 1, :]
            var = jnp.sum(x * z, axis=0, keepdims=True) + cov[4 + p : 5 + p, 4 + p : 5 + p]
            scale = lax.rsqrt(var + 1e-05)
            y = jnp.where(rowt < 4, x8, jnp.where(rowt == 4, 1.0, 0.0)) * scale
            high, mid, low = split3(y)
            right = jnp.concatenate(
                [high, mid, high, mid, low, high, jnp.zeros((80, TILE), jnp.float32)], axis=0
            ).astype(jnp.bfloat16)
            both = jnp.dot(left, right, preferred_element_type=jnp.float32)
            g = both[:hidden]
            v = both[hidden:]
            act = (g * v * (1.0 + lax.erf(g))).astype(jnp.bfloat16)
            got = jnp.dot(inner, act, preferred_element_type=jnp.float32)
            got = got[0:8] + got[8:16]
            per = share // TILE
            part[p, n // per, :, pl.ds(pl.multiple_of(lax.rem(n, per) * TILE, TILE), TILE)] = got[0:4] + got[4:8]
            return carry

        lax.fori_loop(0, pos // TILE, tile, 0, unroll=UNROLL)

    def send_parts(p):
        for k in (1, 2, 3):
            peer = lax.rem(m + k, 4)
            pltpu.make_async_remote_copy(
                src_ref=part.at[p, peer], dst_ref=part_in.at[p, k - 1],
                send_sem=part_send, recv_sem=part_recv.at[p],
                device_id={"tm": i, "mp": peer}, device_id_type=MESH,
            ).start()

    def finish(p):
        pltpu.make_async_copy(part_in.at[p], part_in.at[p], part_recv.at[p]).wait()
        total = part[p, m] + part_in[p, 0] + part_in[p, 1] + part_in[p, 2]
        mine = pl.ds(pl.multiple_of(m * share, share), share)
        cur = lat_ref[p, 0, :, mine]
        nz = noise_ref[p, 0, :, mine]
        for a in range(4):
            total = total + base_row[0:4, a : a + 1] * cur[a : a + 1, :]
        total = total + base_row[0:4, 4 + p : 5 + p]
        eps_ref[p, 0] = total
        c1 = coef[p, 0][0:4]
        c2 = coef[p, 1][0:4]
        c3 = coef[p, 2][0:4]
        head = jnp.where(jnp.full((4, 128), i, jnp.int32) == 0, 1.0, 0.0)
        for s in range(8):
            lanes = slice(s * 128, (s + 1) * 128)
            term = (cur[:, lanes] - c1 * total[:, lanes]) * c2 + c3 * nz[:, lanes] - cur[:, lanes]
            drift[p, :, s // 2, s % 2, :] = term + head * cur[:, lanes]

        def hand_over(n):
            pltpu.make_async_remote_copy(
                src_ref=drift.at[p, n // 4, lax.rem(n, 4)], dst_ref=slots_in.at[p, i],
                send_sem=one_send, recv_sem=one_recv.at[p],
                device_id={"tm": n, "mp": m}, device_id_type=MESH,
            ).start()

        @pl.when(i >= SCANNERS)
        def _():
            for n in range(SCANNERS):
                hand_over(jnp.int32(n))

        @pl.when(i < SCANNERS)
        def _():
            def step(k, carry):
                hand_over(lax.rem(i + k, SCANNERS))
                return carry

            lax.fori_loop(1, SCANNERS, step, 0)
            slots_in[p, SLOTS] = drift[p, i // 4, lax.rem(i, 4)]

    def scan(p):
        settle(slots_in.at[p, pl.ds(0, SLOTS - 1)], one_recv.at[p])
        slots_in[p, i] = slots_in[p, SLOTS]
        acc = slots_in[p, 0]
        sums[1] = acc
        for j in range(1, SLOTS - 1):
            acc = acc + slots_in[p, j]
            sums[j + 1] = acc
        by = slide[p]
        for j in range(SLOTS):
            picked[p, j] = sums[jnp.minimum(j + by, SLOTS - 1)]

        def deliver(k, carry):
            peer = lax.rem(i + k, SLOTS)
            pltpu.make_async_remote_copy(
                src_ref=picked.at[p, peer], dst_ref=whole.at[p, m, i // 4, lax.rem(i, 4)],
                send_sem=two_send, recv_sem=two_recv.at[p],
                device_id={"tm": peer, "mp": m}, device_id_type=MESH,
            ).start()
            return carry

        lax.fori_loop(1, SLOTS, deliver, 0)
        whole[p, m, i // 4, lax.rem(i, 4)] = picked[p, i]

    def settle(ref, sem):
        pltpu.make_async_copy(ref, ref, sem).wait()

    denoise(0)

    @pl.when(i < SCANNERS)
    def _():
        pl.semaphore_wait(barrier, SCANNERS - 1 + 3)

    @pl.when(i >= SCANNERS)
    def _():
        pl.semaphore_wait(barrier, SCANNERS + 3)

    send_parts(0)
    for p in range(1, prompts):
        denoise(p)
        send_parts(p)
        finish(p - 1)
    finish(prompts - 1)

    @pl.when(i < SCANNERS)
    def _():
        for p in range(prompts):
            scan(p)

    for p in range(prompts):

        @pl.when(i < SCANNERS)
        def _():
            settle(slots_in.at[p, pl.ds(0, SCANNERS - 1)], two_recv.at[p])

        @pl.when(i >= SCANNERS)
        def _():
            settle(slots_in.at[p, pl.ds(0, SCANNERS)], two_recv.at[p])

        for k in (1, 2, 3):
            peer = lax.rem(m + k, 4)
            pltpu.make_async_remote_copy(
                src_ref=whole.at[p, m], dst_ref=whole.at[p, m],
                send_sem=all_send, recv_sem=all_recv.at[p],
                device_id={"tm": i, "mp": peer}, device_id_type=MESH,
            ).start()

    for p in range(prompts):
        pltpu.make_async_copy(
            whole.at[p, pl.ds(0, 3)], whole.at[p, pl.ds(0, 3)], all_recv.at[p]
        ).wait()
        for q in range(4):
            for s in range(8):
                out_ref[p, 0, :, q * share + s * 128 : q * share + (s + 1) * 128] = whole[p, q, :, s // 2, s % 2, :]

    settle(part_in, part_send)
    settle(whole.at[:, pl.ds(0, 3)], all_send)

    @pl.when(i < SCANNERS)
    def _():
        settle(slots_in.at[:, pl.ds(0, SLOTS - 1)], two_send)
        settle(slots_in.at[:, pl.ds(0, SCANNERS - 1)], one_send)

    @pl.when(i >= SCANNERS)
    def _():
        settle(slots_in.at[:, pl.ds(0, SCANNERS)], one_send)


def shards(latents, noise, start_step, slide, w_in, w_gate, w_value, w_down, w_out):
    prompts, _, lats, pos = latents.shape
    hidden = w_gate.shape[1]
    share = pos // 4
    f32 = jnp.float32
    smem = pl.BlockSpec(memory_space=pltpu.SMEM)
    vmem = pl.BlockSpec(memory_space=pltpu.VMEM)
    dma = pltpu.SemaphoreType.DMA
    return pl.pallas_call(
        sweep,
        out_shape=(
            jax.ShapeDtypeStruct(latents.shape, f32),
            jax.ShapeDtypeStruct((prompts, 1, lats, share), f32),
        ),
        in_specs=[smem, smem] + [vmem] * 7,
        out_specs=(vmem, vmem),
        scratch_shapes=[
            pltpu.VMEM((prompts, 2 * hidden, 128), jnp.bfloat16),
            pltpu.VMEM((16, hidden), jnp.bfloat16),
            pltpu.VMEM((8, 8), f32),
            pltpu.VMEM((8, 8), f32),
            pltpu.VMEM((prompts, 3, 8, 128), f32),
            pltpu.VMEM((prompts, 4, lats, share), f32),
            pltpu.VMEM((prompts, 3, lats, share), f32),
            pltpu.VMEM((prompts, lats, 4, 2, 128), f32),
            pltpu.VMEM((prompts, SLOTS + 1, 2, 128), f32),
            pltpu.VMEM((SLOTS, 2, 128), f32),
            pltpu.VMEM((prompts, SLOTS, 2, 128), f32),
            pltpu.VMEM((prompts, 4, lats, 4, 2, 128), f32),
            dma, dma((prompts,)), dma, dma((prompts,)), dma, dma((prompts,)), dma, dma((prompts,)),
        ],
        compiler_params=pltpu.CompilerParams(collective_id=0, has_side_effects=True),
        name="sweep",
    )(start_step, slide, latents, noise, w_in, w_gate, w_value, w_down, w_out.T)


def solution(mesh):
    in_specs = (
        P(None, "tm", None, None),
        P(None, "tm", None, None),
        P(),
        P(),
        P(),
        P(None, "mp"),
        P(None, "mp"),
        P("mp", None),
        P(),
    )
    out_specs = (P(None, "tm", None, None), P(None, "tm", None, "mp"))
    return jax.shard_map(shards, mesh=mesh, in_specs=in_specs, out_specs=out_specs, check_vma=False)
```

```python
import functools
import math

import jax
import jax.numpy as jnp
from jax import lax
from jax.experimental import pallas as pl
from jax.experimental.pallas import tpu as pltpu
from jax.sharding import PartitionSpec as P

TSTEPS = 1000
TILE = 2048
UNROLL = 2
SLOTS = 64
SCANNERS = 16
HIGHEST = lax.Precision.HIGHEST
MESH = pl.DeviceIdType.MESH


def split3(x):
    high = x.astype(jnp.bfloat16).astype(jnp.float32)
    rest = x - high
    mid = rest.astype(jnp.bfloat16).astype(jnp.float32)
    return high, mid, rest - mid


def contract_last(a, b):
    return lax.dot_general(
        a, b, (((1,), (1,)), ((), ())), precision=HIGHEST, preferred_element_type=jnp.float32
    )


def product_all(x):
    for axis, extent in ((1, 128), (0, 8)):
        step = 1
        while step < extent:
            x = x * pltpu.roll(x, step, axis)
            step *= 2
    return x


def sweep(
    start, slide, lat_ref, noise_ref, w_in_ref, w_gate_ref, w_value_ref, w_down_ref, w_out_ref,
    out_ref, eps_ref,
    lhs, down, base_row, gram, coef, part, part_in, drift, slots_in, sums, picked, whole,
    part_send, part_recv, one_send, one_recv, two_send, two_recv, all_send, all_recv,
):
    prompts, _, lats, pos = lat_ref.shape
    channels = w_in_ref.shape[1]
    hidden = w_gate_ref.shape[1]
    share = pos // 4
    i = lax.axis_index("tm")
    m = lax.axis_index("mp")

    barrier = pltpu.get_barrier_semaphore()

    def greet(k, carry):
        pl.semaphore_signal(
            barrier, inc=1, device_id={"tm": lax.rem(i + k, SLOTS), "mp": m}, device_id_type=MESH
        )
        return carry

    for k in (1, 2, 3):
        pl.semaphore_signal(
            barrier, inc=1, device_id={"tm": i, "mp": lax.rem(m + k, 4)}, device_id_type=MESH
        )

    @pl.when(i < SCANNERS)
    def _():
        lax.fori_loop(1, SLOTS, greet, 0)

    row8 = lax.broadcasted_iota(jnp.int32, (8, channels), 0)
    lane8 = lax.broadcasted_iota(jnp.int32, (8, channels), 1)
    half = channels // 2
    steps = jnp.zeros((8, channels), jnp.int32)
    for p in range(prompts):
        steps = jnp.where(row8 == 4 + p, start[p] - i, steps)
    freq = jnp.exp(
        -math.log(10000.0) * jnp.where(lane8 < half, lane8, lane8 - half).astype(jnp.float32) / half
    )
    angle = steps.astype(jnp.float32) * freq
    emb = jnp.where(lane8 < half, jnp.cos(angle), jnp.sin(angle))
    w_in = w_in_ref[...]
    rows = jnp.where(row8 < 4, jnp.concatenate([w_in, w_in], axis=0), emb)
    centred = rows - jnp.mean(rows, axis=1, keepdims=True)
    gram[...] = contract_last(centred, centred) * (1.0 / channels)

    w_out = w_out_ref[...]
    w_out_t = jnp.where(row8 < 4, jnp.concatenate([w_out, w_out], axis=0), 0.0)
    base_row[...] = contract_last(w_out_t, rows)

    def three_rows(x):
        return jnp.concatenate(split3(x) + (jnp.zeros_like(x),), axis=0).astype(jnp.bfloat16)

    rowk = lax.broadcasted_iota(jnp.int32, (8, hidden), 0)
    lefts = three_rows(centred)
    tables = []
    for w_ref in (w_gate_ref, w_value_ref):
        pieces = jnp.dot(lefts, w_ref[...], preferred_element_type=jnp.float32)
        tables.append((pieces[0:8] + pieces[8:16] + pieces[16:24]) * math.sqrt(0.5))
    pieces = lax.dot_general(
        three_rows(w_out_t), w_down_ref[...], (((1,), (1,)), ((), ())),
        preferred_element_type=jnp.float32,
    )
    folded = pieces[0:8] + pieces[8:16] + pieces[16:24]
    high, mid, low = split3(folded)
    down[...] = jnp.concatenate(
        [jnp.where(rowk < 4, high, pltpu.roll(mid, 4, 0)), low], axis=0
    ).astype(jnp.bfloat16)

    for p in range(prompts):
        for q, table in enumerate(tables):
            own = jnp.where(
                rowk < 4, table, jnp.where(rowk == 4, table[4 + p : 5 + p, :], 0.0)
            )
            high, mid, low = split3(own)
            stack = jnp.concatenate(
                [high, high, mid, mid, high, low, jnp.zeros((80, hidden), jnp.float32)], axis=0
            )
            turned = jnp.transpose(stack).astype(jnp.bfloat16)
            lhs[p, :, q] = turned.reshape(hidden // 16, 16, 128)

    grid = (
        lax.broadcasted_iota(jnp.int32, (8, 128), 0) * 128
        + lax.broadcasted_iota(jnp.int32, (8, 128), 1)
    )

    def beta_at(k):
        return 0.0001 + (0.02 - 0.0001) * k.astype(jnp.float32) / (TSTEPS - 1)

    kept = 1.0 - beta_at(grid)
    for p in range(prompts):
        t = jnp.full((8, 128), start[p] - i, jnp.int32)
        abar = product_all(jnp.where(grid <= t, kept, 1.0))
        beta = beta_at(t)
        coef[p, 0] = beta / jnp.sqrt(1.0 - abar)
        coef[p, 1] = 1.0 / jnp.sqrt(1.0 - beta)
        coef[p, 2] = jnp.sqrt(beta)

    rowt = lax.broadcasted_iota(jnp.int32, (8, TILE), 0)

    def denoise(p):
        cov = gram[...]
        left = lhs[p].reshape(2 * hidden, 128)
        inner = down[...]

        def tile(n, carry):
            off = pl.multiple_of(n * TILE, TILE)
            x4 = lat_ref[p, 0, :, pl.ds(off, TILE)]
            x8 = jnp.concatenate([x4, x4], axis=0)
            x = jnp.where(rowt < 4, x8, 0.0)
            z = jnp.zeros((8, TILE), jnp.float32) + 2.0 * cov[:, 4 + p : 5 + p]
            for b in range(4):
                z = z + cov[:, b : b + 1] * x4[b : b + 1, :]
            var = jnp.sum(x * z, axis=0, keepdims=True) + cov[4 + p : 5 + p, 4 + p : 5 + p]
            scale = lax.rsqrt(var + 1e-05)
            y = jnp.where(rowt < 4, x8, jnp.where(rowt == 4, 1.0, 0.0)) * scale
            high, mid, low = split3(y)
            right = jnp.concatenate(
                [high, mid, high, mid, low, high, jnp.zeros((80, TILE), jnp.float32)], axis=0
            ).astype(jnp.bfloat16)
            both = jnp.dot(left, right, preferred_element_type=jnp.float32)
            both = both.reshape(hidden // 16, 2, 16, TILE)
            g = both[:, 0]
            v = both[:, 1]
            act = (g * v * (1.0 + lax.erf(g))).astype(jnp.bfloat16).reshape(hidden, TILE)
            got = jnp.dot(inner, act, preferred_element_type=jnp.float32)
            got = got[0:8] + got[8:16]
            per = TILE // share
            for u in range(per):
                w = got[:, u * share : (u + 1) * share]
                part[p, n * per + u] = w[0:4] + w[4:8]
            return carry

        lax.fori_loop(0, pos // TILE, tile, 0, unroll=UNROLL)

    def send_parts(p):
        for k in (1, 2, 3):
            peer = lax.rem(m + k, 4)
            pltpu.make_async_remote_copy(
                src_ref=part.at[p, peer], dst_ref=part_in.at[p, k - 1],
                send_sem=part_send, recv_sem=part_recv.at[p],
                device_id={"tm": i, "mp": peer}, device_id_type=MESH,
            ).start()

    def finish(p):
        pltpu.make_async_copy(part_in.at[p], part_in.at[p], part_recv.at[p]).wait()
        total = part[p, m] + part_in[p, 0] + part_in[p, 1] + part_in[p, 2]
        mine = pl.ds(pl.multiple_of(m * share, share), share)
        cur = lat_ref[p, 0, :, mine]
        nz = noise_ref[p, 0, :, mine]
        for a in range(4):
            total = total + base_row[0:4, a : a + 1] * cur[a : a + 1, :]
        total = total + base_row[0:4, 4 + p : 5 + p]
        eps_ref[p, 0] = total
        c1 = coef[p, 0][0:4]
        c2 = coef[p, 1][0:4]
        c3 = coef[p, 2][0:4]
        head = jnp.where(jnp.full((4, 128), i, jnp.int32) == 0, 1.0, 0.0)
        for s in range(8):
            lanes = slice(s * 128, (s + 1) * 128)
            term = (cur[:, lanes] - c1 * total[:, lanes]) * c2 + c3 * nz[:, lanes] - cur[:, lanes]
            drift[p, :, s // 2, s % 2, :] = term + head * cur[:, lanes]

        def hand_over(n):
            pltpu.make_async_remote_copy(
                src_ref=drift.at[p, n // 4, lax.rem(n, 4)], dst_ref=slots_in.at[p, i],
                send_sem=one_send, recv_sem=one_recv.at[p],
                device_id={"tm": n, "mp": m}, device_id_type=MESH,
            ).start()

        @pl.when(i >= SCANNERS)
        def _():
            for n in range(SCANNERS):
                hand_over(jnp.int32(n))

        @pl.when(i < SCANNERS)
        def _():
            def step(k, carry):
                hand_over(lax.rem(i + k, SCANNERS))
                return carry

            lax.fori_loop(1, SCANNERS, step, 0)
            slots_in[p, SLOTS] = drift[p, i // 4, lax.rem(i, 4)]

    def scan(p):
        settle(slots_in.at[p, pl.ds(0, SLOTS - 1)], one_recv.at[p])
        slots_in[p, i] = slots_in[p, SLOTS]
        acc = slots_in[p, 0]
        sums[1] = acc
        for j in range(1, SLOTS - 1):
            acc = acc + slots_in[p, j]
            sums[j + 1] = acc
        by = slide[p]
        for j in range(SLOTS):
            picked[p, j] = sums[jnp.minimum(j + by, SLOTS - 1)]

        def deliver(k, carry):
            peer = lax.rem(i + k, SLOTS)
            pltpu.make_async_remote_copy(
                src_ref=picked.at[p, peer], dst_ref=whole.at[p, m, i // 4, lax.rem(i, 4)],
                send_sem=two_send, recv_sem=two_recv.at[p],
                device_id={"tm": peer, "mp": m}, device_id_type=MESH,
            ).start()
            return carry

        lax.fori_loop(1, SLOTS, deliver, 0)
        whole[p, m, i // 4, lax.rem(i, 4)] = picked[p, i]

    def settle(ref, sem):
        pltpu.make_async_copy(ref, ref, sem).wait()

    denoise(0)

    @pl.when(i < SCANNERS)
    def _():
        pl.semaphore_wait(barrier, SCANNERS - 1 + 3)

    @pl.when(i >= SCANNERS)
    def _():
        pl.semaphore_wait(barrier, SCANNERS + 3)

    send_parts(0)
    for p in range(1, prompts):
        denoise(p)
        send_parts(p)
        finish(p - 1)
    finish(prompts - 1)

    @pl.when(i < SCANNERS)
    def _():
        for p in range(prompts):
            scan(p)

    for p in range(prompts):

        @pl.when(i < SCANNERS)
        def _():
            settle(slots_in.at[p, pl.ds(0, SCANNERS - 1)], two_recv.at[p])

        @pl.when(i >= SCANNERS)
        def _():
            settle(slots_in.at[p, pl.ds(0, SCANNERS)], two_recv.at[p])

        for k in (1, 2, 3):
            peer = lax.rem(m + k, 4)
            pltpu.make_async_remote_copy(
                src_ref=whole.at[p, m], dst_ref=whole.at[p, m],
                send_sem=all_send, recv_sem=all_recv.at[p],
                device_id={"tm": i, "mp": peer}, device_id_type=MESH,
            ).start()

    for p in range(prompts):
        pltpu.make_async_copy(
            whole.at[p, pl.ds(0, 3)], whole.at[p, pl.ds(0, 3)], all_recv.at[p]
        ).wait()
        for q in range(4):
            for s in range(8):
                out_ref[p, 0, :, q * share + s * 128 : q * share + (s + 1) * 128] = whole[p, q, :, s // 2, s % 2, :]

    settle(part_in, part_send)
    settle(whole.at[:, pl.ds(0, 3)], all_send)

    @pl.when(i < SCANNERS)
    def _():
        settle(slots_in.at[:, pl.ds(0, SLOTS - 1)], two_send)
        settle(slots_in.at[:, pl.ds(0, SCANNERS - 1)], one_send)

    @pl.when(i >= SCANNERS)
    def _():
        settle(slots_in.at[:, pl.ds(0, SCANNERS)], one_send)


def shards(latents, noise, start_step, slide, w_in, w_gate, w_value, w_down, w_out):
    prompts, _, lats, pos = latents.shape
    hidden = w_gate.shape[1]
    share = pos // 4
    f32 = jnp.float32
    smem = pl.BlockSpec(memory_space=pltpu.SMEM)
    vmem = pl.BlockSpec(memory_space=pltpu.VMEM)
    dma = pltpu.SemaphoreType.DMA
    return pl.pallas_call(
        sweep,
        out_shape=(
            pltpu.VMEM(latents.shape, f32),
            pltpu.VMEM((prompts, 1, lats, share), f32),
        ),
        in_specs=[smem, smem] + [vmem] * 7,
        out_specs=(vmem, vmem),
        scratch_shapes=[
            pltpu.VMEM((prompts, hidden // 16, 2, 16, 128), jnp.bfloat16),
            pltpu.VMEM((16, hidden), jnp.bfloat16),
            pltpu.VMEM((8, 8), f32),
            pltpu.VMEM((8, 8), f32),
            pltpu.VMEM((prompts, 3, 8, 128), f32),
            pltpu.VMEM((prompts, 4, lats, share), f32),
            pltpu.VMEM((prompts, 3, lats, share), f32),
            pltpu.VMEM((prompts, lats, 4, 2, 128), f32),
            pltpu.VMEM((prompts, SLOTS + 1, 2, 128), f32),
            pltpu.VMEM((SLOTS, 2, 128), f32),
            pltpu.VMEM((prompts, SLOTS, 2, 128), f32),
            pltpu.VMEM((prompts, 4, lats, 4, 2, 128), f32),
            dma, dma((prompts,)), dma, dma((prompts,)), dma, dma((prompts,)), dma, dma((prompts,)),
        ],
        compiler_params=pltpu.CompilerParams(collective_id=0, has_side_effects=True),
        name="sweep",
    )(start_step, slide, latents, noise, w_in, w_gate, w_value, w_down, w_out.T)


def solution(mesh):
    in_specs = (
        P(None, "tm", None, None),
        P(None, "tm", None, None),
        P(),
        P(),
        P(),
        P(None, "mp"),
        P(None, "mp"),
        P("mp", None),
        P(),
    )
    out_specs = (P(None, "tm", None, None), P(None, "tm", None, "mp"))
    return jax.shard_map(shards, mesh=mesh, in_specs=in_specs, out_specs=out_specs, check_vma=False)
```

```python
import functools
import math

import jax
import jax.numpy as jnp
from jax import lax
from jax.experimental import pallas as pl
from jax.experimental.pallas import tpu as pltpu
from jax.sharding import PartitionSpec as P

TSTEPS = 1000
TILE = 2048
SLOTS = 64
SCANNERS = 8
NEAR = 16
EARLY = 2
HIGHEST = lax.Precision.HIGHEST
MESH = pl.DeviceIdType.MESH


def split3(x):
    high = x.astype(jnp.bfloat16).astype(jnp.float32)
    rest = x - high
    mid = rest.astype(jnp.bfloat16).astype(jnp.float32)
    return high, mid, rest - mid


def contract_last(a, b):
    return lax.dot_general(
        a, b, (((1,), (1,)), ((), ())), precision=HIGHEST, preferred_element_type=jnp.float32
    )


def product_all(x):
    for axis, extent in ((1, 128), (0, 8)):
        step = 1
        while step < extent:
            x = x * pltpu.roll(x, step, axis)
            step *= 2
    return x


def sweep(
    start, slide, lat_ref, noise_ref, w_in_ref, w_gate_ref, w_value_ref, w_down_ref, w_out_ref,
    out_ref, eps_ref,
    lhs, down, rights, scaled, begun, table, table_in, base_row, gram, coef, part, part_in, drift, slots_in, sums, picked, whole,
    table_send, table_recv, part_send, part_recv, one_send, one_recv, two_send, two_recv, all_send, all_recv,
):
    prompts, _, lats, pos = lat_ref.shape
    channels = w_in_ref.shape[1]
    hidden = w_gate_ref.shape[1]
    share = pos // 4
    i = lax.axis_index("tm")
    m = lax.axis_index("mp")
    turn = i // 2
    scanning = jnp.logical_and(lax.rem(i, 2) == 1, i < 2 * SCANNERS)
    resting = jnp.logical_not(scanning)
    own_lat = turn // 2
    own_half = lax.rem(turn, 2)

    barrier = pltpu.get_barrier_semaphore()

    def greet(k, carry):
        pl.semaphore_signal(
            barrier, inc=1, device_id={"tm": lax.rem(i + k, SLOTS), "mp": m}, device_id_type=MESH
        )
        return carry

    for k in (1, 2, 3):
        pl.semaphore_signal(
            barrier, inc=1, device_id={"tm": i, "mp": lax.rem(m + k, 4)}, device_id_type=MESH
        )

    @pl.when(scanning)
    def _():
        lax.fori_loop(1, SLOTS, greet, 0)

    row8 = lax.broadcasted_iota(jnp.int32, (8, channels), 0)
    lane8 = lax.broadcasted_iota(jnp.int32, (8, channels), 1)
    half = channels // 2
    steps = jnp.zeros((8, channels), jnp.int32)
    for p in range(prompts):
        steps = jnp.where(row8 == 4 + p, start[p] - i, steps)
    freq = jnp.exp(
        -math.log(10000.0) * jnp.where(lane8 < half, lane8, lane8 - half).astype(jnp.float32) / half
    )
    angle = steps.astype(jnp.float32) * freq
    emb = jnp.where(lane8 < half, jnp.cos(angle), jnp.sin(angle))
    w_in = w_in_ref[...]
    rows = jnp.where(row8 < 4, jnp.concatenate([w_in, w_in], axis=0), emb)
    centred = rows - jnp.mean(rows, axis=1, keepdims=True)
    gram[...] = contract_last(centred, centred) * (1.0 / channels)

    w_out = w_out_ref[...]
    w_out_t = jnp.where(row8 < 4, jnp.concatenate([w_out, w_out], axis=0), 0.0)
    base_row[...] = contract_last(w_out_t, rows)

    def three_rows(x):
        return jnp.concatenate(split3(x) + (jnp.zeros_like(x),), axis=0).astype(jnp.bfloat16)

    rowk = lax.broadcasted_iota(jnp.int32, (8, hidden), 0)
    lefts = three_rows(centred)
    tables = []
    for w_ref in (w_gate_ref, w_value_ref):
        pieces = jnp.dot(lefts, w_ref[...], preferred_element_type=jnp.float32)
        tables.append((pieces[0:8] + pieces[8:16] + pieces[16:24]) * math.sqrt(0.5))
    pieces = lax.dot_general(
        three_rows(w_out_t), w_down_ref[...], (((1,), (1,)), ((), ())),
        preferred_element_type=jnp.float32,
    )
    folded = pieces[0:8] + pieces[8:16] + pieces[16:24]
    table[0:8] = jnp.where(rowk < 4, tables[0], pltpu.roll(tables[1], 4, 0))
    gates = pltpu.roll(tables[0], 8 - 4 - EARLY, 0)
    values = pltpu.roll(tables[1], 8 - 4 - EARLY + 2, 0)
    table[8:16] = jnp.where(
        rowk < 2, gates, jnp.where(rowk < 4, values, pltpu.roll(folded, 4, 0))
    )

    @pl.when(scanning)
    def _():
        pl.semaphore_wait(barrier, SCANNERS - 1 + 3)

    @pl.when(resting)
    def _():
        pl.semaphore_wait(barrier, SCANNERS + 3)

    for k in (1, 2, 3):
        pltpu.make_async_remote_copy(
            src_ref=table, dst_ref=table_in.at[k - 1],
            send_sem=table_send, recv_sem=table_recv,
            device_id={"tm": i, "mp": lax.rem(m + k, 4)}, device_id_type=MESH,
        ).start()

    def set_left(place, p, gate, value, folded):
        own = jnp.where(rowk < 4, gate, jnp.where(rowk == 4, gate[4 + p : 5 + p, :], 0.0))
        high, mid, low = split3(own)
        stack = jnp.concatenate(
            [high, high, mid, mid, high, low, jnp.zeros((80, hidden), jnp.float32)], axis=0
        )
        turned = jnp.transpose(stack).astype(jnp.bfloat16)
        lhs[place] = turned.reshape(hidden // 16, 16, 128)
        twice = jnp.where(rowk < 4, folded, pltpu.roll(folded, 4, 0))
        levels = [split3(twice * value[r : r + 1, :]) for r in (0, 1, 2, 3, 4 + p)]
        blocks = [levels[r][level] for level in range(3) for r in range(5)]
        blocks.append(jnp.zeros_like(twice))
        down[place] = jnp.concatenate(
            [jnp.where(rowk < 4, blocks[2 * j], blocks[2 * j + 1]) for j in range(8)], axis=0
        ).astype(jnp.bfloat16)

    def place_of(p, k):
        return p if p < EARLY else EARLY + 4 * (p - EARLY) + k

    for p in range(prompts):
        set_left(place_of(p, 0), p, tables[0], tables[1], folded)

    grid = (
        lax.broadcasted_iota(jnp.int32, (8, 128), 0) * 128
        + lax.broadcasted_iota(jnp.int32, (8, 128), 1)
    )

    def beta_at(k):
        return 0.0001 + (0.02 - 0.0001) * k.astype(jnp.float32) / (TSTEPS - 1)

    kept = 1.0 - beta_at(grid)
    for p in range(prompts):
        t = jnp.full((8, 128), start[p] - i, jnp.int32)
        abar = product_all(jnp.where(grid <= t, kept, 1.0))
        beta = beta_at(t)
        coef[p, 0] = beta / jnp.sqrt(1.0 - abar)
        coef[p, 1] = 1.0 / jnp.sqrt(1.0 - beta)
        coef[p, 2] = jnp.sqrt(beta)

    def rescaled(p, x4):
        cov = gram[...]
        width = x4.shape[1]
        rowt = lax.broadcasted_iota(jnp.int32, (8, width), 0)
        x8 = jnp.concatenate([x4, x4], axis=0)
        x = jnp.where(rowt < 4, x8, 0.0)
        z = jnp.zeros((8, width), jnp.float32) + 2.0 * cov[:, 4 + p : 5 + p]
        for b in range(4):
            z = z + cov[:, b : b + 1] * x4[b : b + 1, :]
        var = jnp.sum(x * z, axis=0, keepdims=True) + cov[4 + p : 5 + p, 4 + p : 5 + p]
        scale = lax.rsqrt(var + 1e-05)
        y = jnp.where(rowt < 4, x8, jnp.where(rowt == 4, 1.0, 0.0)) * scale
        high, mid, low = split3(y)
        right = jnp.concatenate(
            [high, mid, high, mid, low, high, jnp.zeros((80, width), jnp.float32)], axis=0
        ).astype(jnp.bfloat16)
        return y, right

    def through(place, right):
        left = lhs[place].reshape(hidden, 128)
        g = jnp.dot(left, right, preferred_element_type=jnp.float32)
        act = (g * (1.0 + lax.erf(g))).astype(jnp.bfloat16)
        return jnp.dot(down[place], act, preferred_element_type=jnp.float32)

    def weighed(got, y):
        rowt = lax.broadcasted_iota(jnp.int32, y.shape, 0)
        total = jnp.zeros_like(y)
        for j in range(8):
            a, b = 2 * j % 5, (2 * j + 1) % 5
            total = total + got[8 * j : 8 * j + 8] * jnp.where(rowt < 4, y[a : a + 1], y[b : b + 1])
        return total[0:4] + total[4:8]

    def denoise(p, n):
        y, right = rescaled(p, lat_ref[p, 0, :, n * TILE : (n + 1) * TILE])
        got = weighed(through(p, right), y)
        per = TILE // share
        for u in range(per):
            part[p, n * per + u] = got[:, u * share : (u + 1) * share]

    def denoise_first(p):
        mine = pl.ds(pl.multiple_of(m * share, share), share)
        y, right = rescaled(p, lat_ref[p, 0, :, mine])
        rights[p - EARLY] = right
        scaled[p - EARLY] = y
        begun[p - EARLY] = through(place_of(p, 0), right)

    def denoise_rest(p):
        total = begun[p - EARLY]
        for k in (1, 2, 3):
            total = total + through(place_of(p, k), rights[p - EARLY])
        return weighed(total, scaled[p - EARLY])

    def take_tables():
        settle(table_in, table_recv)
        for k in (1, 2, 3):
            common, rest = table_in[k - 1, 0:8], table_in[k - 1, 8:16]
            folded = pltpu.roll(rest, 4, 0)
            turned = pltpu.roll(common, 4, 0)
            for p in range(EARLY, prompts):
                n = p - EARLY
                gate = jnp.where(rowk < 4, common, rest[n : n + 1])
                value = jnp.where(rowk < 4, turned, rest[2 + n : 3 + n])
                set_left(place_of(p, k), p, gate, value, folded)

    def send_parts(p):
        for k in (1, 2, 3):
            peer = lax.rem(m + k, 4)
            pltpu.make_async_remote_copy(
                src_ref=part.at[p, peer], dst_ref=part_in.at[p, k - 1],
                send_sem=part_send, recv_sem=part_recv.at[p],
                device_id={"tm": i, "mp": peer}, device_id_type=MESH,
            ).start()

    def summed(p):
        settle(part_in.at[p], part_recv.at[p])
        return part[p, m] + part_in[p, 0] + part_in[p, 1] + part_in[p, 2]

    def finish(p, total):
        mine = pl.ds(pl.multiple_of(m * share, share), share)
        cur = lat_ref[p, 0, :, mine]
        nz = noise_ref[p, 0, :, mine]
        for a in range(4):
            total = total + base_row[0:4, a : a + 1] * cur[a : a + 1, :]
        total = total + base_row[0:4, 4 + p : 5 + p]
        eps_ref[p, 0] = total
        c1 = coef[p, 0][0:4]
        c2 = coef[p, 1][0:4]
        c3 = coef[p, 2][0:4]
        head = jnp.where(jnp.full((4, 128), i, jnp.int32) == 0, 1.0, 0.0)
        for s in range(8):
            lanes = slice(s * 128, (s + 1) * 128)
            term = (cur[:, lanes] - c1 * total[:, lanes]) * c2 + c3 * nz[:, lanes] - cur[:, lanes]
            drift[p, :, s // 4, s % 4, :] = term + head * cur[:, lanes]

        def hand_over(n):
            pltpu.make_async_remote_copy(
                src_ref=drift.at[p, n // 2, lax.rem(n, 2)], dst_ref=slots_in.at[p, i],
                send_sem=one_send, recv_sem=one_recv.at[p],
                device_id={"tm": 2 * n + 1, "mp": m}, device_id_type=MESH,
            ).start()

        @pl.when(resting)
        def _():
            for n in range(SCANNERS):
                hand_over(jnp.int32(n))

        @pl.when(scanning)
        def _():
            def step(k, carry):
                hand_over(lax.rem(turn + k, SCANNERS))
                return carry

            lax.fori_loop(1, SCANNERS, step, 0)
            slots_in[p, SLOTS] = drift[p, own_lat, own_half]

    def deliver(p, low, high):
        def step(peer, carry):
            pltpu.make_async_remote_copy(
                src_ref=picked.at[p, peer], dst_ref=whole.at[p, m, own_lat, own_half],
                send_sem=two_send, recv_sem=two_recv.at[p],
                device_id={"tm": peer, "mp": m}, device_id_type=MESH,
            ).start()
            return carry

        lax.fori_loop(low, high, step, 0)

    def scan(p):
        settle(slots_in.at[p, pl.ds(0, SLOTS - 1)], one_recv.at[p])
        slots_in[p, i] = slots_in[p, SLOTS]
        acc = slots_in[p, 0]
        sums[1] = acc
        for j in range(1, SLOTS - 1):
            acc = acc + slots_in[p, j]
            sums[j + 1] = acc
        by = slide[p]
        for j in range(SLOTS):
            picked[p, j] = sums[jnp.minimum(j + by, SLOTS - 1)]

        deliver(p, 0, i)
        deliver(p, i + 1, NEAR)
        whole[p, m, own_lat, own_half] = picked[p, i]

    def settle(ref, sem):
        pltpu.make_async_copy(ref, ref, sem).wait()

    for p in range(EARLY):
        for n in range(pos // TILE):
            denoise(p, n)
        send_parts(p)
    for p in range(EARLY, prompts):
        denoise_first(p)
    take_tables()
    finish(2, denoise_rest(2))
    finish(0, summed(0))
    finish(1, summed(1))
    finish(3, denoise_rest(3))

    @pl.when(scanning)
    def _():
        scan(2)
        deliver(2, NEAR, SLOTS)
        scan(0)
        deliver(0, NEAR, SLOTS)
        scan(1)
        scan(3)
        deliver(1, NEAR, SLOTS)
        deliver(3, NEAR, SLOTS)

    for p in (2, 0, 1, 3):

        @pl.when(scanning)
        def _():
            settle(slots_in.at[p, pl.ds(0, SCANNERS - 1)], two_recv.at[p])

        @pl.when(resting)
        def _():
            settle(slots_in.at[p, pl.ds(0, SCANNERS)], two_recv.at[p])

        for k in (1, 2, 3):
            peer = lax.rem(m + k, 4)
            pltpu.make_async_remote_copy(
                src_ref=whole.at[p, m], dst_ref=whole.at[p, m],
                send_sem=all_send, recv_sem=all_recv.at[p],
                device_id={"tm": i, "mp": peer}, device_id_type=MESH,
            ).start()

    for p in range(prompts):
        pltpu.make_async_copy(
            whole.at[p, pl.ds(0, 3)], whole.at[p, pl.ds(0, 3)], all_recv.at[p]
        ).wait()
        for q in range(4):
            for s in range(8):
                out_ref[p, 0, :, q * share + s * 128 : q * share + (s + 1) * 128] = whole[p, q, :, s // 4, s % 4, :]

    settle(part_in, part_send)
    settle(table_in, table_send)
    settle(whole.at[:, pl.ds(0, 3)], all_send)

    @pl.when(scanning)
    def _():
        settle(slots_in.at[:, pl.ds(0, SLOTS - 1)], two_send)
        settle(slots_in.at[:, pl.ds(0, SCANNERS - 1)], one_send)

    @pl.when(resting)
    def _():
        settle(slots_in.at[:, pl.ds(0, SCANNERS)], one_send)


def shards(latents, noise, start_step, slide, w_in, w_gate, w_value, w_down, w_out):
    prompts, _, lats, pos = latents.shape
    hidden = w_gate.shape[1]
    share = pos // 4
    f32 = jnp.float32
    smem = pl.BlockSpec(memory_space=pltpu.SMEM)
    vmem = pl.BlockSpec(memory_space=pltpu.VMEM)
    dma = pltpu.SemaphoreType.DMA
    return pl.pallas_call(
        sweep,
        out_shape=(
            pltpu.VMEM(latents.shape, f32),
            pltpu.VMEM((prompts, 1, lats, share), f32),
        ),
        in_specs=[smem, smem] + [vmem] * 7,
        out_specs=(vmem, vmem),
        scratch_shapes=[
            pltpu.VMEM((EARLY + 4 * (prompts - EARLY), hidden // 16, 16, 128), jnp.bfloat16),
            pltpu.VMEM((EARLY + 4 * (prompts - EARLY), 64, hidden), jnp.bfloat16),
            pltpu.VMEM((prompts - EARLY, 128, share), jnp.bfloat16),
            pltpu.VMEM((prompts - EARLY, 8, share), f32),
            pltpu.VMEM((prompts - EARLY, 64, share), f32),
            pltpu.VMEM((16, hidden), f32),
            pltpu.VMEM((3, 16, hidden), f32),
            pltpu.VMEM((8, 8), f32),
            pltpu.VMEM((8, 8), f32),
            pltpu.VMEM((prompts, 3, 8, 128), f32),
            pltpu.VMEM((EARLY, 4, lats, share), f32),
            pltpu.VMEM((EARLY, 3, lats, share), f32),
            pltpu.VMEM((prompts, lats, 2, 4, 128), f32),
            pltpu.VMEM((prompts, SLOTS + 1, 4, 128), f32),
            pltpu.VMEM((SLOTS, 4, 128), f32),
            pltpu.VMEM((prompts, SLOTS, 4, 128), f32),
            pltpu.VMEM((prompts, 4, lats, 2, 4, 128), f32),
            dma, dma, dma, dma((EARLY,)), dma, dma((prompts,)), dma, dma((prompts,)), dma, dma((prompts,)),
        ],
        compiler_params=pltpu.CompilerParams(collective_id=0, has_side_effects=True),
        name="sweep",
    )(start_step, slide, latents, noise, w_in, w_gate, w_value, w_down, w_out.T)


def solution(mesh):
    in_specs = (
        P(None, "tm", None, None),
        P(None, "tm", None, None),
        P(),
        P(),
        P(),
        P(None, "mp"),
        P(None, "mp"),
        P("mp", None),
        P(),
    )
    out_specs = (P(None, "tm", None, None), P(None, "tm", None, "mp"))
    return jax.shard_map(shards, mesh=mesh, in_specs=in_specs, out_specs=out_specs, check_vma=False)
```

```python
import functools
import math

import jax
import jax.numpy as jnp
from jax import lax
from jax.experimental import pallas as pl
from jax.experimental.pallas import tpu as pltpu
from jax.sharding import PartitionSpec as P

TSTEPS = 1000
TILE = 2048
SLOTS = 64
SCANNERS = 8
NEAR = 16
EARLY = 2
HIGHEST = lax.Precision.HIGHEST
MESH = pl.DeviceIdType.MESH


def split3(x):
    high = x.astype(jnp.bfloat16).astype(jnp.float32)
    rest = x - high
    mid = rest.astype(jnp.bfloat16).astype(jnp.float32)
    return high, mid, rest - mid


def contract_last(a, b):
    return lax.dot_general(
        a, b, (((1,), (1,)), ((), ())), precision=HIGHEST, preferred_element_type=jnp.float32
    )


def product_all(x):
    for axis, extent in ((1, 128), (0, 8)):
        step = 1
        while step < extent:
            x = x * pltpu.roll(x, step, axis)
            step *= 2
    return x


def sweep(
    start, slide, lat_ref, noise_ref, w_in_ref, w_gate_ref, w_value_ref, w_down_ref, w_out_ref,
    out_ref, eps_ref,
    lhs, down, rights, scaled, begun, table, table_in, base_row, gram, coef, part, part_in, drift, slots_in, sums, picked, whole,
    table_send, table_recv, part_send, part_recv, one_send, one_recv, two_send, two_recv, all_send, all_recv,
):
    prompts, _, lats, pos = lat_ref.shape
    channels = w_in_ref.shape[1]
    hidden = w_gate_ref.shape[1]
    share = pos // 4
    i = lax.axis_index("tm")
    m = lax.axis_index("mp")
    turn = i // 2
    scanning = jnp.logical_and(lax.rem(i, 2) == 1, i < 2 * SCANNERS)
    resting = jnp.logical_not(scanning)
    own_lat = turn // 2
    own_half = lax.rem(turn, 2)

    barrier = pltpu.get_barrier_semaphore()

    def greet(k, carry):
        pl.semaphore_signal(
            barrier, inc=1, device_id={"tm": lax.rem(i + k, SLOTS), "mp": m}, device_id_type=MESH
        )
        return carry

    for k in (1, 2, 3):
        pl.semaphore_signal(
            barrier, inc=1, device_id={"tm": i, "mp": lax.rem(m + k, 4)}, device_id_type=MESH
        )

    @pl.when(scanning)
    def _():
        lax.fori_loop(1, SLOTS, greet, 0)

    row8 = lax.broadcasted_iota(jnp.int32, (8, channels), 0)
    lane8 = lax.broadcasted_iota(jnp.int32, (8, channels), 1)
    half = channels // 2
    steps = jnp.zeros((8, channels), jnp.int32)
    for p in range(prompts):
        steps = jnp.where(row8 == 4 + p, start[p] - i, steps)
    freq = jnp.exp(
        -math.log(10000.0) * jnp.where(lane8 < half, lane8, lane8 - half).astype(jnp.float32) / half
    )
    angle = steps.astype(jnp.float32) * freq
    emb = jnp.where(lane8 < half, jnp.cos(angle), jnp.sin(angle))
    w_in = w_in_ref[...]
    rows = jnp.where(row8 < 4, jnp.concatenate([w_in, w_in], axis=0), emb)
    centred = rows - jnp.mean(rows, axis=1, keepdims=True)
    gram[...] = contract_last(centred, centred) * (1.0 / channels)

    w_out = w_out_ref[...]
    w_out_t = jnp.where(row8 < 4, jnp.concatenate([w_out, w_out], axis=0), 0.0)
    base_row[...] = contract_last(w_out_t, rows)

    def three_rows(x):
        return jnp.concatenate(split3(x) + (jnp.zeros_like(x),), axis=0).astype(jnp.bfloat16)

    rowk = lax.broadcasted_iota(jnp.int32, (8, hidden), 0)
    lefts = three_rows(centred)
    tables = []
    for w_ref in (w_gate_ref, w_value_ref):
        pieces = jnp.dot(lefts, w_ref[...], preferred_element_type=jnp.float32)
        tables.append((pieces[0:8] + pieces[8:16] + pieces[16:24]) * math.sqrt(0.5))
    pieces = lax.dot_general(
        three_rows(w_out_t), w_down_ref[...], (((1,), (1,)), ((), ())),
        preferred_element_type=jnp.float32,
    )
    folded = pieces[0:8] + pieces[8:16] + pieces[16:24]
    table[0:8] = jnp.where(rowk < 4, tables[0], pltpu.roll(tables[1], 4, 0))
    gates = pltpu.roll(tables[0], 8 - 4 - EARLY, 0)
    values = pltpu.roll(tables[1], 8 - 4 - EARLY + 2, 0)
    table[8:16] = jnp.where(
        rowk < 2, gates, jnp.where(rowk < 4, values, pltpu.roll(folded, 4, 0))
    )

    @pl.when(scanning)
    def _():
        pl.semaphore_wait(barrier, SCANNERS - 1 + 3)

    @pl.when(resting)
    def _():
        pl.semaphore_wait(barrier, SCANNERS + 3)

    for k in (1, 2, 3):
        pltpu.make_async_remote_copy(
            src_ref=table, dst_ref=table_in.at[k - 1],
            send_sem=table_send, recv_sem=table_recv,
            device_id={"tm": i, "mp": lax.rem(m + k, 4)}, device_id_type=MESH,
        ).start()

    def set_left(place, p, gate, value, folded):
        own = jnp.where(rowk < 4, gate, jnp.where(rowk == 4, gate[4 + p : 5 + p, :], 0.0))
        high, mid, low = split3(own)
        stack = jnp.concatenate(
            [high, high, mid, mid, high, low, jnp.zeros((80, hidden), jnp.float32)], axis=0
        )
        turned = jnp.transpose(stack).astype(jnp.bfloat16)
        lhs[place] = turned.reshape(hidden // 16, 16, 128)
        twice = jnp.where(rowk < 4, folded, pltpu.roll(folded, 4, 0))
        levels = [split3(twice * value[r : r + 1, :]) for r in (0, 1, 2, 3, 4 + p)]
        blocks = [levels[r][level] for level in range(3) for r in range(5)]
        blocks.append(jnp.zeros_like(twice))
        down[place] = jnp.concatenate(
            [jnp.where(rowk < 4, blocks[2 * j], blocks[2 * j + 1]) for j in range(8)], axis=0
        ).astype(jnp.bfloat16)

    def place_of(p, k):
        return p if p < EARLY else EARLY + 4 * (p - EARLY) + k

    for p in range(prompts):
        set_left(place_of(p, 0), p, tables[0], tables[1], folded)

    grid = (
        lax.broadcasted_iota(jnp.int32, (8, 128), 0) * 128
        + lax.broadcasted_iota(jnp.int32, (8, 128), 1)
    )

    def beta_at(k):
        return 0.0001 + (0.02 - 0.0001) * k.astype(jnp.float32) / (TSTEPS - 1)

    kept = 1.0 - beta_at(grid)
    for p in range(prompts):
        t = jnp.full((8, 128), start[p] - i, jnp.int32)
        abar = product_all(jnp.where(grid <= t, kept, 1.0))
        beta = beta_at(t)
        coef[p, 0] = beta / jnp.sqrt(1.0 - abar)
        coef[p, 1] = 1.0 / jnp.sqrt(1.0 - beta)
        coef[p, 2] = jnp.sqrt(beta)

    def rescaled(p, x4):
        cov = gram[...]
        width = x4.shape[1]
        rowt = lax.broadcasted_iota(jnp.int32, (8, width), 0)
        x8 = jnp.concatenate([x4, x4], axis=0)
        x = jnp.where(rowt < 4, x8, 0.0)
        z = jnp.zeros((8, width), jnp.float32) + 2.0 * cov[:, 4 + p : 5 + p]
        for b in range(4):
            z = z + cov[:, b : b + 1] * x4[b : b + 1, :]
        var = jnp.sum(x * z, axis=0, keepdims=True) + cov[4 + p : 5 + p, 4 + p : 5 + p]
        scale = lax.rsqrt(var + 1e-05)
        y = jnp.where(rowt < 4, x8, jnp.where(rowt == 4, 1.0, 0.0)) * scale
        high, mid, low = split3(y)
        right = jnp.concatenate(
            [high, mid, high, mid, low, high, jnp.zeros((80, width), jnp.float32)], axis=0
        ).astype(jnp.bfloat16)
        return y, right

    def through(place, right):
        left = lhs[place].reshape(hidden, 128)
        g = jnp.dot(left, right, preferred_element_type=jnp.float32)
        act = (g * (1.0 + lax.erf(g))).astype(jnp.bfloat16)
        return jnp.dot(down[place], act, preferred_element_type=jnp.float32)

    def weighed(got, y):
        rowt = lax.broadcasted_iota(jnp.int32, y.shape, 0)
        total = jnp.zeros_like(y)
        for j in range(8):
            a, b = 2 * j % 5, (2 * j + 1) % 5
            total = total + got[8 * j : 8 * j + 8] * jnp.where(rowt < 4, y[a : a + 1], y[b : b + 1])
        return total[0:4] + total[4:8]

    def denoise(p, n):
        y, right = rescaled(p, lat_ref[p, 0, :, n * TILE : (n + 1) * TILE])
        got = weighed(through(p, right), y)
        per = TILE // share
        for u in range(per):
            part[p, n * per + u] = got[:, u * share : (u + 1) * share]

    def denoise_first(p):
        mine = pl.ds(pl.multiple_of(m * share, share), share)
        y, right = rescaled(p, lat_ref[p, 0, :, mine])
        rights[p - EARLY] = right
        scaled[p - EARLY] = y
        begun[p - EARLY] = through(place_of(p, 0), right)

    def denoise_rest(p):
        total = begun[p - EARLY]
        for k in (1, 2, 3):
            total = total + through(place_of(p, k), rights[p - EARLY])
        return weighed(total, scaled[p - EARLY])

    def take_tables():
        settle(table_in, table_recv)
        for k in (1, 2, 3):
            common, rest = table_in[k - 1, 0:8], table_in[k - 1, 8:16]
            folded = pltpu.roll(rest, 4, 0)
            turned = pltpu.roll(common, 4, 0)
            for p in range(EARLY, prompts):
                n = p - EARLY
                gate = jnp.where(rowk < 4, common, rest[n : n + 1])
                value = jnp.where(rowk < 4, turned, rest[2 + n : 3 + n])
                set_left(place_of(p, k), p, gate, value, folded)

    def send_parts(p):
        for k in (1, 2, 3):
            peer = lax.rem(m + k, 4)
            pltpu.make_async_remote_copy(
                src_ref=part.at[p, peer], dst_ref=part_in.at[p, k - 1],
                send_sem=part_send, recv_sem=part_recv.at[p],
                device_id={"tm": i, "mp": peer}, device_id_type=MESH,
            ).start()

    def summed(p):
        settle(part_in.at[p], part_recv.at[p])
        return part[p, m] + part_in[p, 0] + part_in[p, 1] + part_in[p, 2]

    def finish(p, total):
        mine = pl.ds(pl.multiple_of(m * share, share), share)
        cur = lat_ref[p, 0, :, mine]
        nz = noise_ref[p, 0, :, mine]
        for a in range(4):
            total = total + base_row[0:4, a : a + 1] * cur[a : a + 1, :]
        total = total + base_row[0:4, 4 + p : 5 + p]
        eps_ref[p, 0] = total
        c1 = coef[p, 0][0:4]
        c2 = coef[p, 1][0:4]
        c3 = coef[p, 2][0:4]
        head = jnp.where(jnp.full((4, 128), i, jnp.int32) == 0, 1.0, 0.0)
        for s in range(8):
            lanes = slice(s * 128, (s + 1) * 128)
            term = (cur[:, lanes] - c1 * total[:, lanes]) * c2 + c3 * nz[:, lanes] - cur[:, lanes]
            drift[p, :, s // 4, s % 4, :] = term + head * cur[:, lanes]

        def hand_over(n):
            pltpu.make_async_remote_copy(
                src_ref=drift.at[p, n // 2, lax.rem(n, 2)], dst_ref=slots_in.at[p, i],
                send_sem=one_send, recv_sem=one_recv.at[p],
                device_id={"tm": 2 * n + 1, "mp": m}, device_id_type=MESH,
            ).start()

        @pl.when(resting)
        def _():
            for n in range(SCANNERS):
                hand_over(jnp.int32(n))

        @pl.when(scanning)
        def _():
            def step(k, carry):
                hand_over(lax.rem(turn + k, SCANNERS))
                return carry

            lax.fori_loop(1, SCANNERS, step, 0)
            slots_in[p, SLOTS] = drift[p, own_lat, own_half]

    def deliver(p, low, high):
        def step(peer, carry):
            pltpu.make_async_remote_copy(
                src_ref=picked.at[p, peer], dst_ref=whole.at[p, m, own_lat, own_half],
                send_sem=two_send, recv_sem=two_recv.at[p],
                device_id={"tm": peer, "mp": m}, device_id_type=MESH,
            ).start()
            return carry

        lax.fori_loop(low, high, step, 0)

    def scan(p):
        settle(slots_in.at[p, pl.ds(0, SLOTS - 1)], one_recv.at[p])
        slots_in[p, i] = slots_in[p, SLOTS]
        acc = slots_in[p, 0]
        sums[1] = acc
        for j in range(1, SLOTS - 1):
            acc = acc + slots_in[p, j]
            sums[j + 1] = acc
        by = slide[p]
        for j in range(SLOTS):
            picked[p, j] = sums[jnp.minimum(j + by, SLOTS - 1)]

        deliver(p, 0, i)
        deliver(p, i + 1, NEAR)
        whole[p, m, own_lat, own_half] = picked[p, i]

    def settle(ref, sem):
        pltpu.make_async_copy(ref, ref, sem).wait()

    for p in range(EARLY):
        for n in range(pos // TILE):
            denoise(p, n)
        send_parts(p)
    for p in range(EARLY, prompts):
        denoise_first(p)
    take_tables()
    finish(2, denoise_rest(2))
    finish(0, summed(0))
    finish(1, summed(1))
    finish(3, denoise_rest(3))

    @pl.when(scanning)
    def _():
        scan(2)
        deliver(2, NEAR, SLOTS)
        scan(0)
        deliver(0, NEAR, SLOTS)
        scan(1)
        scan(3)
        deliver(1, NEAR, SLOTS)
        deliver(3, NEAR, SLOTS)

    for p in (2, 0, 1, 3):

        @pl.when(scanning)
        def _():
            settle(slots_in.at[p, pl.ds(0, SCANNERS - 1)], two_recv.at[p])

        @pl.when(resting)
        def _():
            settle(slots_in.at[p, pl.ds(0, SCANNERS)], two_recv.at[p])

        for k in (1, 2, 3):
            peer = lax.rem(m + k, 4)
            pltpu.make_async_remote_copy(
                src_ref=whole.at[p, m], dst_ref=whole.at[p, m],
                send_sem=all_send, recv_sem=all_recv.at[p],
                device_id={"tm": i, "mp": peer}, device_id_type=MESH,
            ).start()

    for p in range(prompts):
        pltpu.make_async_copy(
            whole.at[p, pl.ds(0, 3)], whole.at[p, pl.ds(0, 3)], all_recv.at[p]
        ).wait()
        for q in range(4):
            for s in range(8):
                out_ref[p, 0, :, q * share + s * 128 : q * share + (s + 1) * 128] = whole[p, q, :, s // 4, s % 4, :]

    settle(part_in, part_send)
    settle(table_in, table_send)
    settle(whole.at[:, pl.ds(0, 3)], all_send)

    @pl.when(scanning)
    def _():
        settle(slots_in.at[:, pl.ds(0, SLOTS - 1)], two_send)
        settle(slots_in.at[:, pl.ds(0, SCANNERS - 1)], one_send)

    @pl.when(resting)
    def _():
        settle(slots_in.at[:, pl.ds(0, SCANNERS)], one_send)


def put_out(window, eps, window_out, eps_out, sems):
    copies = [
        pltpu.make_async_copy(window, window_out, sems.at[0]),
        pltpu.make_async_copy(eps, eps_out, sems.at[1]),
    ]
    for copy in copies:
        copy.start()
    for copy in copies:
        copy.wait()


def shards(latents, noise, start_step, slide, w_in, w_gate, w_value, w_down, w_out):
    prompts, _, lats, pos = latents.shape
    hidden = w_gate.shape[1]
    share = pos // 4
    f32 = jnp.float32
    smem = pl.BlockSpec(memory_space=pltpu.SMEM)
    vmem = pl.BlockSpec(memory_space=pltpu.VMEM)
    any_space = pl.BlockSpec(memory_space=pl.ANY)
    dma = pltpu.SemaphoreType.DMA
    window, eps = pl.pallas_call(
        sweep,
        out_shape=(
            pltpu.VMEM(latents.shape, f32),
            pltpu.VMEM((prompts, 1, lats, share), f32),
        ),
        in_specs=[smem, smem] + [vmem] * 7,
        out_specs=(vmem, vmem),
        scratch_shapes=[
            pltpu.VMEM((EARLY + 4 * (prompts - EARLY), hidden // 16, 16, 128), jnp.bfloat16),
            pltpu.VMEM((EARLY + 4 * (prompts - EARLY), 64, hidden), jnp.bfloat16),
            pltpu.VMEM((prompts - EARLY, 128, share), jnp.bfloat16),
            pltpu.VMEM((prompts - EARLY, 8, share), f32),
            pltpu.VMEM((prompts - EARLY, 64, share), f32),
            pltpu.VMEM((16, hidden), f32),
            pltpu.VMEM((3, 16, hidden), f32),
            pltpu.VMEM((8, 8), f32),
            pltpu.VMEM((8, 8), f32),
            pltpu.VMEM((prompts, 3, 8, 128), f32),
            pltpu.VMEM((EARLY, 4, lats, share), f32),
            pltpu.VMEM((EARLY, 3, lats, share), f32),
            pltpu.VMEM((prompts, lats, 2, 4, 128), f32),
            pltpu.VMEM((prompts, SLOTS + 1, 4, 128), f32),
            pltpu.VMEM((SLOTS, 4, 128), f32),
            pltpu.VMEM((prompts, SLOTS, 4, 128), f32),
            pltpu.VMEM((prompts, 4, lats, 2, 4, 128), f32),
            dma, dma, dma, dma((EARLY,)), dma, dma((prompts,)), dma, dma((prompts,)), dma, dma((prompts,)),
        ],
        compiler_params=pltpu.CompilerParams(collective_id=0, has_side_effects=True),
        name="sweep",
    )(start_step, slide, latents, noise, w_in, w_gate, w_value, w_down, w_out.T)
    return pl.pallas_call(
        put_out,
        out_shape=(
            jax.ShapeDtypeStruct(latents.shape, f32),
            jax.ShapeDtypeStruct((prompts, 1, lats, share), f32),
        ),
        in_specs=[any_space, any_space],
        out_specs=(any_space, any_space),
        scratch_shapes=[dma((2,))],
        compiler_params=pltpu.CompilerParams(vmem_limit_bytes=1024 * 1024),
        name="put_out",
    )(window, eps)


def solution(mesh):
    in_specs = (
        P(None, "tm", None, None),
        P(None, "tm", None, None),
        P(),
        P(),
        P(),
        P(None, "mp"),
        P(None, "mp"),
        P("mp", None),
        P(),
    )
    out_specs = (P(None, "tm", None, None), P(None, "tm", None, "mp"))
    return jax.shard_map(shards, mesh=mesh, in_specs=in_specs, out_specs=out_specs, check_vma=False)
```

```python
import functools
import math

import jax
import jax.numpy as jnp
from jax import lax
from jax.experimental import pallas as pl
from jax.experimental.pallas import tpu as pltpu
from jax.sharding import PartitionSpec as P

TSTEPS = 1000
TILE = 2048
SLOTS = 64
SCANNERS = 8
HIGHEST = lax.Precision.HIGHEST
MESH = pl.DeviceIdType.MESH


def split3(x):
    high = x.astype(jnp.bfloat16).astype(jnp.float32)
    rest = x - high
    mid = rest.astype(jnp.bfloat16).astype(jnp.float32)
    return high, mid, rest - mid


def contract_last(a, b):
    return lax.dot_general(
        a, b, (((1,), (1,)), ((), ())), precision=HIGHEST, preferred_element_type=jnp.float32
    )


def product_all(x):
    for axis, extent in ((1, 128), (0, 8)):
        step = 1
        while step < extent:
            x = x * pltpu.roll(x, step, axis)
            step *= 2
    return x


def sweep(
    start, slide, lat_ref, noise_ref, w_in_ref, w_gate_ref, w_value_ref, w_down_ref, w_out_ref,
    out_ref, eps_ref,
    lhs, down, base_row, gram, coef, part, part_in, drift, slots_in, sums, picked, whole,
    part_send, part_recv, one_send, one_recv, two_send, two_recv, all_send, all_recv,
):
    prompts, _, lats, pos = lat_ref.shape
    channels = w_in_ref.shape[1]
    hidden = w_gate_ref.shape[1]
    share = pos // 4
    i = lax.axis_index("tm")
    m = lax.axis_index("mp")
    turn = i // 2
    scanning = jnp.logical_and(lax.rem(i, 2) == 1, i < 2 * SCANNERS)
    resting = jnp.logical_not(scanning)
    own_lat = turn // 2
    own_half = lax.rem(turn, 2)

    barrier = pltpu.get_barrier_semaphore()

    def greet(k, carry):
        pl.semaphore_signal(
            barrier, inc=1, device_id={"tm": lax.rem(i + k, SLOTS), "mp": m}, device_id_type=MESH
        )
        return carry

    for k in (1, 2, 3):
        pl.semaphore_signal(
            barrier, inc=1, device_id={"tm": i, "mp": lax.rem(m + k, 4)}, device_id_type=MESH
        )

    @pl.when(scanning)
    def _():
        lax.fori_loop(1, SLOTS, greet, 0)

    row8 = lax.broadcasted_iota(jnp.int32, (8, channels), 0)
    lane8 = lax.broadcasted_iota(jnp.int32, (8, channels), 1)
    half = channels // 2
    steps = jnp.zeros((8, channels), jnp.int32)
    for p in range(prompts):
        steps = jnp.where(row8 == 4 + p, start[p] - i, steps)
    freq = jnp.exp(
        -math.log(10000.0) * jnp.where(lane8 < half, lane8, lane8 - half).astype(jnp.float32) / half
    )
    angle = steps.astype(jnp.float32) * freq
    emb = jnp.where(lane8 < half, jnp.cos(angle), jnp.sin(angle))
    w_in = w_in_ref[...]
    rows = jnp.where(row8 < 4, jnp.concatenate([w_in, w_in], axis=0), emb)
    centred = rows - jnp.mean(rows, axis=1, keepdims=True)
    gram[...] = contract_last(centred, centred) * (1.0 / channels)

    w_out = w_out_ref[...]
    w_out_t = jnp.where(row8 < 4, jnp.concatenate([w_out, w_out], axis=0), 0.0)
    base_row[...] = contract_last(w_out_t, rows)

    def three_rows(x):
        return jnp.concatenate(split3(x) + (jnp.zeros_like(x),), axis=0).astype(jnp.bfloat16)

    rowk = lax.broadcasted_iota(jnp.int32, (8, hidden), 0)
    lefts = three_rows(centred)
    tables = []
    for w_ref in (w_gate_ref, w_value_ref):
        pieces = jnp.dot(lefts, w_ref[...], preferred_element_type=jnp.float32)
        tables.append((pieces[0:8] + pieces[8:16] + pieces[16:24]) * math.sqrt(0.5))
    pieces = lax.dot_general(
        three_rows(w_out_t), w_down_ref[...], (((1,), (1,)), ((), ())),
        preferred_element_type=jnp.float32,
    )
    folded = pieces[0:8] + pieces[8:16] + pieces[16:24]
    def set_left(place, p, gate, value, folded):
        own = jnp.where(rowk < 4, gate, jnp.where(rowk == 4, gate[4 + p : 5 + p, :], 0.0))
        high, mid, low = split3(own)
        stack = jnp.concatenate(
            [high, high, mid, mid, high, low, jnp.zeros((80, hidden), jnp.float32)], axis=0
        )
        turned = jnp.transpose(stack).astype(jnp.bfloat16)
        lhs[place] = turned.reshape(hidden // 16, 16, 128)
        twice = jnp.where(rowk < 4, folded, pltpu.roll(folded, 4, 0))
        levels = [split3(twice * value[r : r + 1, :]) for r in (0, 1, 2, 3, 4 + p)]
        blocks = [levels[r][level] for level in range(3) for r in range(5)]
        blocks.append(jnp.zeros_like(twice))
        down[place] = jnp.concatenate(
            [jnp.where(rowk < 4, blocks[2 * j], blocks[2 * j + 1]) for j in range(8)], axis=0
        ).astype(jnp.bfloat16)

    for p in range(prompts):
        set_left(p, p, tables[0], tables[1], folded)

    grid = (
        lax.broadcasted_iota(jnp.int32, (8, 128), 0) * 128
        + lax.broadcasted_iota(jnp.int32, (8, 128), 1)
    )

    def beta_at(k):
        return 0.0001 + (0.02 - 0.0001) * k.astype(jnp.float32) / (TSTEPS - 1)

    kept = 1.0 - beta_at(grid)
    for p in range(prompts):
        t = jnp.full((8, 128), start[p] - i, jnp.int32)
        abar = product_all(jnp.where(grid <= t, kept, 1.0))
        beta = beta_at(t)
        coef[p, 0] = beta / jnp.sqrt(1.0 - abar)
        coef[p, 1] = 1.0 / jnp.sqrt(1.0 - beta)
        coef[p, 2] = jnp.sqrt(beta)

    def rescaled(p, x4):
        cov = gram[...]
        width = x4.shape[1]
        rowt = lax.broadcasted_iota(jnp.int32, (8, width), 0)
        x8 = jnp.concatenate([x4, x4], axis=0)
        x = jnp.where(rowt < 4, x8, 0.0)
        z = jnp.zeros((8, width), jnp.float32) + 2.0 * cov[:, 4 + p : 5 + p]
        for b in range(4):
            z = z + cov[:, b : b + 1] * x4[b : b + 1, :]
        var = jnp.sum(x * z, axis=0, keepdims=True) + cov[4 + p : 5 + p, 4 + p : 5 + p]
        scale = lax.rsqrt(var + 1e-05)
        y = jnp.where(rowt < 4, x8, jnp.where(rowt == 4, 1.0, 0.0)) * scale
        high, mid, low = split3(y)
        right = jnp.concatenate(
            [high, mid, high, mid, low, high, jnp.zeros((80, width), jnp.float32)], axis=0
        ).astype(jnp.bfloat16)
        return y, right

    def through(place, right):
        left = lhs[place].reshape(hidden, 128)
        g = jnp.dot(left, right, preferred_element_type=jnp.float32)
        act = (g * (1.0 + lax.erf(g))).astype(jnp.bfloat16)
        return jnp.dot(down[place], act, preferred_element_type=jnp.float32)

    def weighed(got, y):
        rowt = lax.broadcasted_iota(jnp.int32, y.shape, 0)
        total = jnp.zeros_like(y)
        for j in range(8):
            a, b = 2 * j % 5, (2 * j + 1) % 5
            total = total + got[8 * j : 8 * j + 8] * jnp.where(rowt < 4, y[a : a + 1], y[b : b + 1])
        return total[0:4] + total[4:8]

    def denoise(p, n):
        y, right = rescaled(p, lat_ref[p, 0, :, n * TILE : (n + 1) * TILE])
        got = weighed(through(p, right), y)
        per = TILE // share
        for u in range(per):
            part[p, n * per + u] = got[:, u * share : (u + 1) * share]

    def send_parts(p):
        for k in (2, 1, 3):
            peer = lax.rem(m + k, 4)
            pltpu.make_async_remote_copy(
                src_ref=part.at[p, peer], dst_ref=part_in.at[p, k - 1],
                send_sem=part_send, recv_sem=part_recv.at[p],
                device_id={"tm": i, "mp": peer}, device_id_type=MESH,
            ).start()

    def summed(p):
        settle(part_in.at[p], part_recv.at[p])
        return part[p, m] + part_in[p, 0] + part_in[p, 1] + part_in[p, 2]

    def finish(p, total):
        mine = pl.ds(pl.multiple_of(m * share, share), share)
        cur = lat_ref[p, 0, :, mine]
        nz = noise_ref[p, 0, :, mine]
        for a in range(4):
            total = total + base_row[0:4, a : a + 1] * cur[a : a + 1, :]
        total = total + base_row[0:4, 4 + p : 5 + p]
        eps_ref[p, 0] = total
        c1 = coef[p, 0][0:4]
        c2 = coef[p, 1][0:4]
        c3 = coef[p, 2][0:4]
        head = jnp.where(jnp.full((4, 128), i, jnp.int32) == 0, 1.0, 0.0)
        for s in range(8):
            lanes = slice(s * 128, (s + 1) * 128)
            term = (cur[:, lanes] - c1 * total[:, lanes]) * c2 + c3 * nz[:, lanes] - cur[:, lanes]
            drift[p, :, s // 4, s % 4, :] = term + head * cur[:, lanes]

        def hand_over(n):
            pltpu.make_async_remote_copy(
                src_ref=drift.at[p, n // 2, lax.rem(n, 2)], dst_ref=slots_in.at[p, i],
                send_sem=one_send, recv_sem=one_recv.at[p],
                device_id={"tm": 2 * n + 1, "mp": m}, device_id_type=MESH,
            ).start()

        @pl.when(resting)
        def _():
            for n in range(SCANNERS):
                hand_over(jnp.int32(n))

        @pl.when(scanning)
        def _():
            def step(k, carry):
                hand_over(lax.rem(turn + k, SCANNERS))
                return carry

            lax.fori_loop(1, SCANNERS, step, 0)
            slots_in[p, SLOTS] = drift[p, own_lat, own_half]

    def scan(p):
        settle(slots_in.at[p, pl.ds(0, SLOTS - 1)], one_recv.at[p])
        slots_in[p, i] = slots_in[p, SLOTS]
        acc = slots_in[p, 0]
        sums[1] = acc
        for j in range(1, SLOTS - 1):
            acc = acc + slots_in[p, j]
            sums[j + 1] = acc
        by = slide[p]
        for j in range(SLOTS):
            picked[p, j] = sums[jnp.minimum(j + by, SLOTS - 1)]

        def deliver(peer, carry):
            pltpu.make_async_remote_copy(
                src_ref=picked.at[p, peer], dst_ref=whole.at[p, m, own_lat, own_half],
                send_sem=two_send, recv_sem=two_recv.at[p],
                device_id={"tm": peer, "mp": m}, device_id_type=MESH,
            ).start()
            return carry

        lax.fori_loop(0, i, deliver, 0)
        lax.fori_loop(i + 1, SLOTS, deliver, 0)
        whole[p, m, own_lat, own_half] = picked[p, i]

    def settle(ref, sem):
        pltpu.make_async_copy(ref, ref, sem).wait()

    for p in range(prompts):
        for n in range(pos // TILE):
            denoise(p, n)
        if p == 0:

                @pl.when(scanning)
                def _():
                    pl.semaphore_wait(barrier, SCANNERS - 1 + 3)

                @pl.when(resting)
                def _():
                    pl.semaphore_wait(barrier, SCANNERS + 3)

        send_parts(p)
        if p == prompts - 1:
            finish(0, summed(0))
    for p in range(1, prompts):
        finish(p, summed(p))

    @pl.when(scanning)
    def _():
        for p in range(prompts):
            scan(p)

    for p in range(prompts):

        @pl.when(scanning)
        def _():
            settle(slots_in.at[p, pl.ds(0, SCANNERS - 1)], two_recv.at[p])

        @pl.when(resting)
        def _():
            settle(slots_in.at[p, pl.ds(0, SCANNERS)], two_recv.at[p])

        for k in (2, 1, 3):
            peer = lax.rem(m + k, 4)
            pltpu.make_async_remote_copy(
                src_ref=whole.at[p, m], dst_ref=whole.at[p, m],
                send_sem=all_send, recv_sem=all_recv.at[p],
                device_id={"tm": i, "mp": peer}, device_id_type=MESH,
            ).start()

    for p in range(prompts):
        pltpu.make_async_copy(
            whole.at[p, pl.ds(0, 3)], whole.at[p, pl.ds(0, 3)], all_recv.at[p]
        ).wait()
        for q in range(4):
            for s in range(8):
                out_ref[p, 0, :, q * share + s * 128 : q * share + (s + 1) * 128] = whole[p, q, :, s // 4, s % 4, :]

    settle(part_in, part_send)
    settle(whole.at[:, pl.ds(0, 3)], all_send)

    @pl.when(scanning)
    def _():
        settle(slots_in.at[:, pl.ds(0, SLOTS - 1)], two_send)
        settle(slots_in.at[:, pl.ds(0, SCANNERS - 1)], one_send)

    @pl.when(resting)
    def _():
        settle(slots_in.at[:, pl.ds(0, SCANNERS)], one_send)


def put_out(window, eps, window_out, eps_out, sems):
    copies = [
        pltpu.make_async_copy(window, window_out, sems.at[0]),
        pltpu.make_async_copy(eps, eps_out, sems.at[1]),
    ]
    for copy in copies:
        copy.start()
    for copy in copies:
        copy.wait()


def shards(latents, noise, start_step, slide, w_in, w_gate, w_value, w_down, w_out):
    prompts, _, lats, pos = latents.shape
    hidden = w_gate.shape[1]
    share = pos // 4
    f32 = jnp.float32
    smem = pl.BlockSpec(memory_space=pltpu.SMEM)
    vmem = pl.BlockSpec(memory_space=pltpu.VMEM)
    any_space = pl.BlockSpec(memory_space=pl.ANY)
    dma = pltpu.SemaphoreType.DMA
    window, eps = pl.pallas_call(
        sweep,
        out_shape=(
            pltpu.VMEM(latents.shape, f32),
            pltpu.VMEM((prompts, 1, lats, share), f32),
        ),
        in_specs=[smem, smem] + [vmem] * 7,
        out_specs=(vmem, vmem),
        scratch_shapes=[
            pltpu.VMEM((prompts, hidden // 16, 16, 128), jnp.bfloat16),
            pltpu.VMEM((prompts, 64, hidden), jnp.bfloat16),
            pltpu.VMEM((8, 8), f32),
            pltpu.VMEM((8, 8), f32),
            pltpu.VMEM((prompts, 3, 8, 128), f32),
            pltpu.VMEM((prompts, 4, lats, share), f32),
            pltpu.VMEM((prompts, 3, lats, share), f32),
            pltpu.VMEM((prompts, lats, 2, 4, 128), f32),
            pltpu.VMEM((prompts, SLOTS + 1, 4, 128), f32),
            pltpu.VMEM((SLOTS, 4, 128), f32),
            pltpu.VMEM((prompts, SLOTS, 4, 128), f32),
            pltpu.VMEM((prompts, 4, lats, 2, 4, 128), f32),
            dma, dma((prompts,)), dma, dma((prompts,)), dma, dma((prompts,)), dma, dma((prompts,)),
        ],
        compiler_params=pltpu.CompilerParams(collective_id=0, has_side_effects=True),
        name="sweep",
    )(start_step, slide, latents, noise, w_in, w_gate, w_value, w_down, w_out.T)
    return pl.pallas_call(
        put_out,
        out_shape=(
            jax.ShapeDtypeStruct(latents.shape, f32),
            jax.ShapeDtypeStruct((prompts, 1, lats, share), f32),
        ),
        in_specs=[any_space, any_space],
        out_specs=(any_space, any_space),
        scratch_shapes=[dma((2,))],
        compiler_params=pltpu.CompilerParams(vmem_limit_bytes=1024 * 1024),
        name="put_out",
    )(window, eps)


def solution(mesh):
    in_specs = (
        P(None, "tm", None, None),
        P(None, "tm", None, None),
        P(),
        P(),
        P(),
        P(None, "mp"),
        P(None, "mp"),
        P("mp", None),
        P(),
    )
    out_specs = (P(None, "tm", None, None), P(None, "tm", None, "mp"))
    return jax.shard_map(shards, mesh=mesh, in_specs=in_specs, out_specs=out_specs, check_vma=False)
```

```python
import functools
import math

import jax
import jax.numpy as jnp
from jax import lax
from jax.experimental import pallas as pl
from jax.experimental.pallas import tpu as pltpu
from jax.sharding import PartitionSpec as P

TSTEPS = 1000
TILE = 2048
SLOTS = 64
SCANNERS = 8
HIGHEST = lax.Precision.HIGHEST
MESH = pl.DeviceIdType.MESH


def split3(x):
    high = x.astype(jnp.bfloat16).astype(jnp.float32)
    rest = x - high
    mid = rest.astype(jnp.bfloat16).astype(jnp.float32)
    return high, mid, rest - mid


def contract_last(a, b):
    return lax.dot_general(
        a, b, (((1,), (1,)), ((), ())), precision=HIGHEST, preferred_element_type=jnp.float32
    )


def product_all(x):
    for axis, extent in ((1, 128), (0, 8)):
        step = 1
        while step < extent:
            x = x * pltpu.roll(x, step, axis)
            step *= 2
    return x


def sweep(
    start, slide, lat_ref, noise_ref, w_in_ref, w_gate_ref, w_value_ref, w_down_ref, w_out_ref,
    out_ref, eps_ref,
    lhs, down, base_row, gram, coef, part, part_in, drift, slots_in, sums, picked, whole,
    part_send, part_recv, one_send, one_recv, two_send, two_recv, all_send, all_recv,
):
    prompts, _, lats, pos = lat_ref.shape
    channels = w_in_ref.shape[1]
    hidden = w_gate_ref.shape[1]
    share = pos // 4
    i = lax.axis_index("tm")
    m = lax.axis_index("mp")
    turn = i // 2
    scanning = jnp.logical_and(lax.rem(i, 2) == 1, i < 2 * SCANNERS)
    resting = jnp.logical_not(scanning)
    own_lat = turn // 2
    own_half = lax.rem(turn, 2)

    barrier = pltpu.get_barrier_semaphore()

    def greet(k, carry):
        pl.semaphore_signal(
            barrier, inc=1, device_id={"tm": lax.rem(i + k, SLOTS), "mp": m}, device_id_type=MESH
        )
        return carry

    for k in (1, 2, 3):
        pl.semaphore_signal(
            barrier, inc=1, device_id={"tm": i, "mp": lax.rem(m + k, 4)}, device_id_type=MESH
        )

    @pl.when(scanning)
    def _():
        lax.fori_loop(1, SLOTS, greet, 0)

    row8 = lax.broadcasted_iota(jnp.int32, (8, channels), 0)
    lane8 = lax.broadcasted_iota(jnp.int32, (8, channels), 1)
    half = channels // 2
    steps = jnp.zeros((8, channels), jnp.int32)
    for p in range(prompts):
        steps = jnp.where(row8 == 4 + p, start[p] - i, steps)
    freq = jnp.exp(
        -math.log(10000.0) * jnp.where(lane8 < half, lane8, lane8 - half).astype(jnp.float32) / half
    )
    angle = steps.astype(jnp.float32) * freq
    emb = jnp.where(lane8 < half, jnp.cos(angle), jnp.sin(angle))
    w_in = w_in_ref[...]
    rows = jnp.where(row8 < 4, jnp.concatenate([w_in, w_in], axis=0), emb)
    centred = rows - jnp.mean(rows, axis=1, keepdims=True)
    gram[...] = contract_last(centred, centred) * (1.0 / channels)

    w_out = w_out_ref[...]
    w_out_t = jnp.where(row8 < 4, jnp.concatenate([w_out, w_out], axis=0), 0.0)
    base_row[...] = contract_last(w_out_t, rows)

    def three_rows(x):
        return jnp.concatenate(split3(x) + (jnp.zeros_like(x),), axis=0).astype(jnp.bfloat16)

    rowk = lax.broadcasted_iota(jnp.int32, (8, hidden), 0)
    lefts = three_rows(centred)
    tables = []
    for w_ref in (w_gate_ref, w_value_ref):
        pieces = jnp.dot(lefts, w_ref[...], preferred_element_type=jnp.float32)
        tables.append((pieces[0:8] + pieces[8:16] + pieces[16:24]) * math.sqrt(0.5))
    pieces = lax.dot_general(
        three_rows(w_out_t), w_down_ref[...], (((1,), (1,)), ((), ())),
        preferred_element_type=jnp.float32,
    )
    folded = pieces[0:8] + pieces[8:16] + pieces[16:24]
    def set_left(place, p, gate, value, folded):
        own = jnp.where(rowk < 4, gate, jnp.where(rowk == 4, gate[4 + p : 5 + p, :], 0.0))
        high, mid, low = split3(own)
        stack = jnp.concatenate(
            [high, high, mid, mid, high, low, jnp.zeros((80, hidden), jnp.float32)], axis=0
        )
        turned = jnp.transpose(stack).astype(jnp.bfloat16)
        lhs[place] = turned.reshape(hidden // 16, 16, 128)
        twice = jnp.where(rowk < 4, folded, pltpu.roll(folded, 4, 0))
        levels = [split3(twice * value[r : r + 1, :]) for r in (0, 1, 2, 3, 4 + p)]
        blocks = [levels[r][level] for level in range(3) for r in range(5)]
        blocks.append(jnp.zeros_like(twice))
        down[place] = jnp.concatenate(
            [jnp.where(rowk < 4, blocks[2 * j], blocks[2 * j + 1]) for j in range(8)], axis=0
        ).astype(jnp.bfloat16)

    for p in range(prompts):
        set_left(p, p, tables[0], tables[1], folded)

    grid = (
        lax.broadcasted_iota(jnp.int32, (8, 128), 0) * 128
        + lax.broadcasted_iota(jnp.int32, (8, 128), 1)
    )

    def beta_at(k):
        return 0.0001 + (0.02 - 0.0001) * k.astype(jnp.float32) / (TSTEPS - 1)

    kept = 1.0 - beta_at(grid)
    for p in range(prompts):
        t = jnp.full((8, 128), start[p] - i, jnp.int32)
        abar = product_all(jnp.where(grid <= t, kept, 1.0))
        beta = beta_at(t)
        coef[p, 0] = beta / jnp.sqrt(1.0 - abar)
        coef[p, 1] = 1.0 / jnp.sqrt(1.0 - beta)
        coef[p, 2] = jnp.sqrt(beta)

    def rescaled(p, x4):
        cov = gram[...]
        width = x4.shape[1]
        rowt = lax.broadcasted_iota(jnp.int32, (8, width), 0)
        x8 = jnp.concatenate([x4, x4], axis=0)
        x = jnp.where(rowt < 4, x8, 0.0)
        z = jnp.zeros((8, width), jnp.float32) + 2.0 * cov[:, 4 + p : 5 + p]
        for b in range(4):
            z = z + cov[:, b : b + 1] * x4[b : b + 1, :]
        var = jnp.sum(x * z, axis=0, keepdims=True) + cov[4 + p : 5 + p, 4 + p : 5 + p]
        scale = lax.rsqrt(jnp.maximum(var, 0.0) + 1e-05)
        y = jnp.where(rowt < 4, x8, jnp.where(rowt == 4, 1.0, 0.0)) * scale
        high, mid, low = split3(y)
        right = jnp.concatenate(
            [high, mid, high, mid, low, high, jnp.zeros((80, width), jnp.float32)], axis=0
        ).astype(jnp.bfloat16)
        return y, right

    def through(place, right):
        left = lhs[place].reshape(hidden, 128)
        g = jnp.dot(left, right, preferred_element_type=jnp.float32)
        act = (g * (1.0 + lax.erf(g))).astype(jnp.bfloat16)
        return jnp.dot(down[place], act, preferred_element_type=jnp.float32)

    def weighed(got, y):
        rowt = lax.broadcasted_iota(jnp.int32, y.shape, 0)
        total = jnp.zeros_like(y)
        for j in range(8):
            a, b = 2 * j % 5, (2 * j + 1) % 5
            total = total + got[8 * j : 8 * j + 8] * jnp.where(rowt < 4, y[a : a + 1], y[b : b + 1])
        return total[0:4] + total[4:8]

    def denoise(p, n):
        y, right = rescaled(p, lat_ref[p, 0, :, n * TILE : (n + 1) * TILE])
        got = weighed(through(p, right), y)
        per = TILE // share
        for u in range(per):
            part[p, n * per + u] = got[:, u * share : (u + 1) * share]

    def send_parts(p):
        for k in (2, 1, 3):
            peer = lax.rem(m + k, 4)
            pltpu.make_async_remote_copy(
                src_ref=part.at[p, peer], dst_ref=part_in.at[p, k - 1],
                send_sem=part_send, recv_sem=part_recv.at[p],
                device_id={"tm": i, "mp": peer}, device_id_type=MESH,
            ).start()

    def summed(p):
        settle(part_in.at[p], part_recv.at[p])
        return part[p, m] + part_in[p, 0] + part_in[p, 1] + part_in[p, 2]

    def finish(p, total):
        mine = pl.ds(pl.multiple_of(m * share, share), share)
        cur = lat_ref[p, 0, :, mine]
        nz = noise_ref[p, 0, :, mine]
        for a in range(4):
            total = total + base_row[0:4, a : a + 1] * cur[a : a + 1, :]
        total = total + base_row[0:4, 4 + p : 5 + p]
        eps_ref[p, 0] = total
        c1 = coef[p, 0][0:4]
        c2 = coef[p, 1][0:4]
        c3 = coef[p, 2][0:4]
        head = jnp.where(jnp.full((4, 128), i, jnp.int32) == 0, 1.0, 0.0)
        for s in range(8):
            lanes = slice(s * 128, (s + 1) * 128)
            term = (cur[:, lanes] - c1 * total[:, lanes]) * c2 + c3 * nz[:, lanes] - cur[:, lanes]
            drift[p, :, s // 4, s % 4, :] = term + head * cur[:, lanes]

        def hand_over(n):
            pltpu.make_async_remote_copy(
                src_ref=drift.at[p, n // 2, lax.rem(n, 2)], dst_ref=slots_in.at[p, i],
                send_sem=one_send, recv_sem=one_recv.at[p],
                device_id={"tm": 2 * n + 1, "mp": m}, device_id_type=MESH,
            ).start()

        @pl.when(resting)
        def _():
            for n in range(SCANNERS):
                hand_over(jnp.int32(n))

        @pl.when(scanning)
        def _():
            def step(k, carry):
                hand_over(lax.rem(turn + k, SCANNERS))
                return carry

            lax.fori_loop(1, SCANNERS, step, 0)
            slots_in[p, SLOTS] = drift[p, own_lat, own_half]

    def scan(p):
        settle(slots_in.at[p, pl.ds(0, SLOTS - 1)], one_recv.at[p])
        slots_in[p, i] = slots_in[p, SLOTS]
        acc = slots_in[p, 0]
        sums[1] = acc
        for j in range(1, SLOTS - 1):
            acc = acc + slots_in[p, j]
            sums[j + 1] = acc
        by = slide[p]
        for j in range(SLOTS):
            picked[p, j] = sums[jnp.minimum(j + by, SLOTS - 1)]

        def deliver(peer, carry):
            pltpu.make_async_remote_copy(
                src_ref=picked.at[p, peer], dst_ref=whole.at[p, m, own_lat, own_half],
                send_sem=two_send, recv_sem=two_recv.at[p],
                device_id={"tm": peer, "mp": m}, device_id_type=MESH,
            ).start()
            return carry

        lax.fori_loop(0, i, deliver, 0)
        lax.fori_loop(i + 1, SLOTS, deliver, 0)
        whole[p, m, own_lat, own_half] = picked[p, i]

    def settle(ref, sem):
        pltpu.make_async_copy(ref, ref, sem).wait()

    for p in range(prompts):
        for n in range(pos // TILE):
            denoise(p, n)
        if p == 0:

                @pl.when(scanning)
                def _():
                    pl.semaphore_wait(barrier, SCANNERS - 1 + 3)

                @pl.when(resting)
                def _():
                    pl.semaphore_wait(barrier, SCANNERS + 3)

        send_parts(p)
        if p == prompts - 1:
            finish(0, summed(0))
    for p in range(1, prompts):
        finish(p, summed(p))

    @pl.when(scanning)
    def _():
        for p in range(prompts):
            scan(p)

    for p in range(prompts):

        @pl.when(scanning)
        def _():
            settle(slots_in.at[p, pl.ds(0, SCANNERS - 1)], two_recv.at[p])

        @pl.when(resting)
        def _():
            settle(slots_in.at[p, pl.ds(0, SCANNERS)], two_recv.at[p])

        for k in (2, 1, 3):
            peer = lax.rem(m + k, 4)
            pltpu.make_async_remote_copy(
                src_ref=whole.at[p, m], dst_ref=whole.at[p, m],
                send_sem=all_send, recv_sem=all_recv.at[p],
                device_id={"tm": i, "mp": peer}, device_id_type=MESH,
            ).start()

    for p in range(prompts):
        pltpu.make_async_copy(
            whole.at[p, pl.ds(0, 3)], whole.at[p, pl.ds(0, 3)], all_recv.at[p]
        ).wait()
        for q in range(4):
            for s in range(8):
                out_ref[p, 0, :, q * share + s * 128 : q * share + (s + 1) * 128] = whole[p, q, :, s // 4, s % 4, :]

    settle(part_in, part_send)
    settle(whole.at[:, pl.ds(0, 3)], all_send)

    @pl.when(scanning)
    def _():
        settle(slots_in.at[:, pl.ds(0, SLOTS - 1)], two_send)
        settle(slots_in.at[:, pl.ds(0, SCANNERS - 1)], one_send)

    @pl.when(resting)
    def _():
        settle(slots_in.at[:, pl.ds(0, SCANNERS)], one_send)


def put_out(window, eps, window_out, eps_out, sems):
    copies = [
        pltpu.make_async_copy(window, window_out, sems.at[0]),
        pltpu.make_async_copy(eps, eps_out, sems.at[1]),
    ]
    for copy in copies:
        copy.start()
    for copy in copies:
        copy.wait()


def shards(latents, noise, start_step, slide, w_in, w_gate, w_value, w_down, w_out):
    prompts, _, lats, pos = latents.shape
    hidden = w_gate.shape[1]
    share = pos // 4
    f32 = jnp.float32
    smem = pl.BlockSpec(memory_space=pltpu.SMEM)
    vmem = pl.BlockSpec(memory_space=pltpu.VMEM)
    any_space = pl.BlockSpec(memory_space=pl.ANY)
    dma = pltpu.SemaphoreType.DMA
    window, eps = pl.pallas_call(
        sweep,
        out_shape=(
            pltpu.VMEM(latents.shape, f32),
            pltpu.VMEM((prompts, 1, lats, share), f32),
        ),
        in_specs=[smem, smem] + [vmem] * 7,
        out_specs=(vmem, vmem),
        scratch_shapes=[
            pltpu.VMEM((prompts, hidden // 16, 16, 128), jnp.bfloat16),
            pltpu.VMEM((prompts, 64, hidden), jnp.bfloat16),
            pltpu.VMEM((8, 8), f32),
            pltpu.VMEM((8, 8), f32),
            pltpu.VMEM((prompts, 3, 8, 128), f32),
            pltpu.VMEM((prompts, 4, lats, share), f32),
            pltpu.VMEM((prompts, 3, lats, share), f32),
            pltpu.VMEM((prompts, lats, 2, 4, 128), f32),
            pltpu.VMEM((prompts, SLOTS + 1, 4, 128), f32),
            pltpu.VMEM((SLOTS, 4, 128), f32),
            pltpu.VMEM((prompts, SLOTS, 4, 128), f32),
            pltpu.VMEM((prompts, 4, lats, 2, 4, 128), f32),
            dma, dma((prompts,)), dma, dma((prompts,)), dma, dma((prompts,)), dma, dma((prompts,)),
        ],
        compiler_params=pltpu.CompilerParams(collective_id=0, has_side_effects=True),
        name="sweep",
    )(start_step, slide, latents, noise, w_in, w_gate, w_value, w_down, w_out.T)
    return pl.pallas_call(
        put_out,
        out_shape=(
            jax.ShapeDtypeStruct(latents.shape, f32),
            jax.ShapeDtypeStruct((prompts, 1, lats, share), f32),
        ),
        in_specs=[any_space, any_space],
        out_specs=(any_space, any_space),
        scratch_shapes=[dma((2,))],
        compiler_params=pltpu.CompilerParams(vmem_limit_bytes=1024 * 1024),
        name="put_out",
    )(window, eps)


def solution(mesh):
    in_specs = (
        P(None, "tm", None, None),
        P(None, "tm", None, None),
        P(),
        P(),
        P(),
        P(None, "mp"),
        P(None, "mp"),
        P("mp", None),
        P(),
    )
    out_specs = (P(None, "tm", None, None), P(None, "tm", None, "mp"))
    return jax.shard_map(shards, mesh=mesh, in_specs=in_specs, out_specs=out_specs, check_vma=False)
```
